32 devices in a mesh: gx: 8 (over z, x), gy: 4 (over y, core).
Axes of the slice: x: 2, y: 2, z: 4, core: 2. Of those that a mesh axis runs over, the one named last changes fastest.
Arguments:
- species: float32 [53, 32, 32, 128], P(None, 'gx', 'gy'), may hold values from -6 to 6
- diffusion: float32 [53], replicated, may hold values from 0.02 to 0.15
- class_rate: float32 [4], replicated, may hold values from 0.2 to 1
- mixing: float32 [53, 53], replicated, may hold values from -0.3 to 0.3
- inverses: float32 [4, 53, 53], replicated, may hold values from -0.01 to 0.12
- newton_counts: int32 [4], replicated, may hold values from 1 to 8, as said below
- cell_class: int32 [32, 32, 128], P('gx', 'gy'), may hold values from 0 to 3
Outputs:
- updated: float32 [53, 32, 32, 128], P(None, 'gx', 'gy')
The draws below stay inside these ranges and needn't reach their ends.
Inputs may be any that keep to these rules, and one draw needn't show every extreme that they name: `newton_counts`: nondecreasing in the class; the last class takes 8.
All inputs are finite; a program needn't handle non-finite values.
Results may differ from the reference program's by a relative error of at most 0.0003.
Values sent between devices are 32-bit elements; how exact they have to be, the bound alone decides.
A program may use at most 64 MiB of HBM per device.

```python
import math
import jax
import jax.numpy as jnp
from jax import lax

SPEC = 53
NCLASS = 4
NMAX = 8
NZ = 128
NX = 32
NY = 32


def draw_inverses(key, part):
    first, second = jax.random.split(jax.random.fold_in(key, 5))
    diag = jnp.exp(jax.random.uniform(first, (NCLASS, SPEC), jnp.float32, math.log(0.06), math.log(0.12)))
    spread = jax.random.normal(second, (NCLASS, SPEC, SPEC), jnp.float32)
    spread = jnp.clip(spread * (0.0225 / math.sqrt(SPEC)), -0.01, 0.01)
    identity = jnp.eye(SPEC, dtype=jnp.float32)[None]
    return spread * (1.0 - identity) + diag[:, :, None] * identity


def draw_newton_counts(key, part):
    base = jax.random.randint(jax.random.fold_in(key, 11), (NCLASS,), 1, NMAX + 1)
    base = jnp.sort(base)
    return base.at[NCLASS - 1].set(NMAX).astype(jnp.int32)


def draw_cell_class(key, part):
    front_key, heavy_key, pick_key, light_key = jax.random.split(jax.random.fold_in(key, 23), 4)
    front = jax.random.randint(front_key, (), 0, NX)
    positions = jnp.arange(NX, dtype=jnp.int32)[:, None, None]
    near = jnp.abs(positions - front) < max(NX // 16, 1)
    shape = (NX, NY, NZ)
    heavy = jax.random.randint(heavy_key, shape, 1, NCLASS)
    picked = jax.random.randint(pick_key, shape, 0, 8)
    light = jnp.where(picked == 0, jax.random.randint(light_key, shape, 0, NCLASS), 0)
    return jnp.where(near, heavy, light).astype(jnp.int32)


def level_of(stream_key, shape, shards, least, largest):
    gain = 1.0
    for dim, shards_of in shards:
        draws = jax.random.uniform(jax.random.fold_in(jax.random.fold_in(stream_key, 6), dim), (shards_of,), jnp.float32, least / len(shards), largest / len(shards))
        gain = gain * jnp.repeat(jnp.exp(draws), shape[dim] // shards_of).reshape((-1,) + (1,) * (len(shape) - 1 - dim))
    return gain


def normal_values(own_key, extent, scale, bound, cuts=(), held_as=jnp.bfloat16):
    level = level_of(own_key, extent, cuts, -0.22, 0.18) if cuts else 1.0
    values = jax.random.normal(own_key, extent, jnp.float32) * scale * level
    return jnp.minimum(jnp.maximum(values, -bound), bound).astype(held_as)


def setup_inputs(seed: int = 0) -> dict:
    arg_keys = jax.random.split(jax.random.key(seed), 8)
    species = normal_values(arg_keys[0], (SPEC, NX, NY, NZ), 1.0, 6.0, ((1, 8), (2, 4)), jnp.float32)
    diffusion = jnp.clip(jnp.exp(jax.random.uniform(arg_keys[1], (SPEC,), jnp.float32, math.log(0.02), math.log(0.15))), 0.02, 0.15)
    class_rate = jnp.clip(jnp.exp(jax.random.uniform(arg_keys[2], (NCLASS,), jnp.float32, math.log(0.2), math.log(1.0))), 0.2, 1.0)
    mixing = normal_values(arg_keys[3], (SPEC, SPEC), (0.3 * SPEC ** -0.5), 0.3, (), jnp.float32)
    inverses = draw_inverses(jax.random.fold_in(arg_keys[7], 71), 0)
    newton_counts = draw_newton_counts(jax.random.fold_in(arg_keys[7], 71), 0)
    cell_class = draw_cell_class(jax.random.fold_in(arg_keys[7], 71), 0)
    return {"species": species, "diffusion": diffusion, "class_rate": class_rate, "mixing": mixing, "inverses": inverses, "newton_counts": newton_counts, "cell_class": cell_class}


def laplace(grid_field):
    padded = jnp.pad(grid_field, 1)
    total = padded[2:, 1:-1, 1:-1] + padded[:-2, 1:-1, 1:-1]
    total = total + padded[1:-1, 2:, 1:-1] + padded[1:-1, :-2, 1:-1]
    total = total + padded[1:-1, 1:-1, 2:] + padded[1:-1, 1:-1, :-2]
    return total - 6.0 * grid_field


def newton_cells(target, classes, class_rate, mixing, inverses, newton_counts):
    class_mask = (classes[None, :] == jnp.arange(NCLASS, dtype=jnp.int32)[:, None])
    weights = class_mask.astype(jnp.float32)
    cell_rate = jnp.sum(class_rate[:, None] * weights, axis=0)
    cell_count = jnp.sum(jnp.where(class_mask, newton_counts[:, None], 0), axis=0)

    def newton_step(k, state):
        source = jnp.dot(mixing, jnp.tanh(state), precision=lax.Precision.HIGHEST) - state
        residual = state - target - cell_rate * source
        correction = jnp.zeros_like(state)
        for which in range(NCLASS):
            correction = correction + weights[which] * jnp.dot(inverses[which], residual, precision=lax.Precision.HIGHEST)
        return jnp.where(k < cell_count, state - correction, state)

    return lax.fori_loop(0, NMAX, newton_step, target)


def reference(species, diffusion, class_rate, mixing, inverses, newton_counts, cell_class):
    forcing = lax.map(laplace, species) * diffusion[:, None, None, None]
    target = species + forcing
    moved = jnp.moveaxis(target, 1, 0)

    def solve_slice(pair):
        slab, slab_class = pair
        solved = newton_cells(slab.reshape(SPEC, -1), slab_class.reshape(-1), class_rate, mixing, inverses, newton_counts)
        return solved.reshape(slab.shape)

    section_value = jnp.moveaxis(lax.map(solve_slice, (moved, cell_class)), 0, 1)
    second = lax.map(laplace, section_value) * diffusion[:, None, None, None]
    return section_value + 0.5 * (second - forcing)
```

```python
import functools

import jax
import jax.numpy as jnp
from jax import lax
from jax.experimental import pallas as pl
from jax.experimental.pallas import tpu as pltpu
from jax.sharding import PartitionSpec as P

NMAX = 8
SPAN = 4
MESH = pl.DeviceIdType.MESH
F32 = jnp.float32
BF16 = jnp.bfloat16


def pairs_of(n):
    return [tuple(sorted({c, n - 1 - c})) for c in range((n + 1) // 2)]


def kernel(
    dims,
    species_hbm, diffusion_hbm, rate_hbm, mixing_hbm, inverses_hbm, counts_hbm, class_hbm,
    out,
    ext, ext2, scaled, coef, row, mix, inv, stack, square, w_high, w_low, classes, rates, counts,
    load_sem, small_sem, xs_send, xs_recv, ys_send, ys_recv,
):
    spec, nx, ny, nz, nclass = dims
    pad = ext.shape[2]
    real = pl.ds(0, spec)
    gx, gy = lax.axis_index("gx"), lax.axis_index("gy")
    sx, sy = lax.axis_size("gx"), lax.axis_size("gy")
    has_x = (gx > 0, gx < sx - 1)
    has_y = (gy > 0, gy < sy - 1)
    to_x = ((gx - 1, gy), (gx + 1, gy))
    to_y = ((gx, gy - 1), (gx, gy + 1))
    edges = pairs_of(ny)

    def load(x, y):
        return pltpu.make_async_copy(
            species_hbm.at[:, x, y], ext.at[x + 1, y + 1, real], load_sem.at[x, y])

    sides = sorted({0, nx - 1})
    first = [(x, y) for y in edges[0] for x in sides]
    first += [(x, y) for y in edges[0] for x in range(1, nx - 1)]
    first += [(x, y) for pair in edges[1:] for y in pair for x in sides]
    later = [(x, y) for pair in edges[1:] for y in pair for x in range(1, nx - 1)]
    for x, y in first + later:
        load(x, y).start()
    small = [
        pltpu.make_async_copy(src, dst, small_sem.at[i]) for i, (src, dst) in enumerate((
            (mixing_hbm, mix), (inverses_hbm, inv), (diffusion_hbm, row),
            (rate_hbm, rates), (counts_hbm, counts), (class_hbm, classes)))]
    for copy in small:
        copy.start()

    barrier = pltpu.get_barrier_semaphore()
    for has, to in zip(has_x + has_y, to_x + to_y):
        @pl.when(has)
        def _():
            pl.semaphore_signal(barrier, inc=1, device_id=to, device_id_type=MESH)

    tail = jnp.zeros((pad - spec, nz), F32)
    for x in range(nx + 2):
        for y in range(ny + 2):
            halo = x in (0, nx + 1) or y in (0, ny + 1)
            if x in (0, nx + 1) and y in (0, ny + 1):
                continue
            ext[x, y, pl.ds(spec, pad - spec)] = tail
            if halo:
                ext2[x, y, pl.ds(spec, pad - spec)] = tail
    blank = jnp.zeros((spec, nz), F32)
    for side in (0, 1):
        @pl.when(jnp.logical_not(has_x[side]))
        def _():
            for buf in (ext, ext2):
                for y in range(ny):
                    buf[side * (nx + 1), y + 1, real] = blank
        @pl.when(jnp.logical_not(has_y[side]))
        def _():
            for buf in (ext, ext2):
                for x in range(nx):
                    buf[x + 1, side * (ny + 1), real] = blank

    def x_copy(stage, side, y):
        buf = (ext, ext2)[stage]
        src_row, dst_row = (1, nx + 1) if side == 0 else (nx, 0)
        return pltpu.make_async_remote_copy(
            src_ref=buf.at[src_row, y + 1, real], dst_ref=buf.at[dst_row, y + 1, real],
            send_sem=xs_send.at[stage, side, y], recv_sem=xs_recv.at[stage, side, y],
            device_id=to_x[side], device_id_type=MESH)

    def y_copy(stage, side):
        buf = (ext, ext2)[stage]
        src_col, dst_col = (1, ny + 1) if side == 0 else (ny, 0)
        return pltpu.make_async_remote_copy(
            src_ref=buf.at[pl.ds(1, nx), src_col, real],
            dst_ref=buf.at[pl.ds(1, nx), dst_col, real],
            send_sem=ys_send.at[stage, side], recv_sem=ys_recv.at[stage, side],
            device_id=to_y[side], device_id_type=MESH)

    def x_start(stage, ys):
        for side in (0, 1):
            @pl.when(has_x[side])
            def _():
                for y in ys:
                    x_copy(stage, side, y).start()

    def x_arrive(stage, ys):
        for side in (0, 1):
            @pl.when(has_x[side])
            def _():
                for y in ys:
                    x_copy(stage, 1 - side, y).wait_recv()

    def y_start(stage):
        for side in (0, 1):
            @pl.when(has_y[side])
            def _():
                y_copy(stage, side).start()

    def y_arrive(stage):
        for side in (0, 1):
            @pl.when(has_y[side])
            def _():
                y_copy(stage, 1 - side).wait_recv()

    neighbours = sum(has.astype(jnp.int32) for has in has_x + has_y)
    pl.semaphore_wait(barrier, neighbours)
    for x, y in first:
        load(x, y).wait()
    x_start(0, edges[0])
    y_start(0)
    for pair in edges[1:]:
        x_start(0, pair)

    for copy in small:
        copy.wait()
    stack[...] = jnp.zeros_like(stack)
    square[...] = jnp.zeros_like(square)
    square[0:1, 0:spec] = row[...]
    line = jnp.broadcast_to(square[0:1, :], square.shape)
    on = lax.broadcasted_iota(jnp.int32, square.shape, 0) == lax.broadcasted_iota(
        jnp.int32, square.shape, 1)
    column = jnp.sum(jnp.where(on, line, 0.0), axis=1, keepdims=True)
    coef[...] = jnp.broadcast_to(column[:pad], coef.shape)
    square[0:spec, 0:spec] = mix[...]
    for k in range(nclass):
        stack[k * pad:k * pad + spec, 0:spec] = inv[:, k, :]
    mixed = jnp.dot(
        stack[...], square[...], precision=lax.Precision.HIGHEST, preferred_element_type=F32)
    spread = lax.broadcasted_iota(jnp.int32, (pad, 128), 1)
    highs, lows = [], []
    for k in range(nclass):
        rate = rates[k]
        own = stack[k * pad:(k + 1) * pad, :] * -(1.0 + rate)
        other = mixed[k * pad:(k + 1) * pad, :] * (rate * (1.0 + rate))
        both = own + pltpu.roll(other, pad, 1)
        high = both.astype(BF16).astype(F32)
        for part, into in ((high, highs), (both - high, lows)):
            turned = pltpu.roll(part, 2 * pad, 1)
            into.append(jnp.concatenate(
                [jnp.where(spread < 2 * pad, part, turned), turned], axis=1))
    for parts, ref in ((highs, w_high), (lows, w_low)):
        ref[...] = jnp.concatenate(
            [parts[k][t * 8:(t + 1) * 8] for t in range(pad // 8) for k in range(nclass)],
            axis=0)[:, :4 * pad].astype(BF16)

    lane = lax.broadcasted_iota(jnp.int32, (pad, nz), 1)

    def laplace(buf, x, y):
        v = buf[x + 1, y + 1]
        total = buf[x + 2, y + 1] + buf[x, y + 1] + buf[x + 1, y + 2] + buf[x + 1, y]
        total = total + jnp.where(lane == nz - 1, 0.0, pltpu.roll(v, nz - 1, 1))
        total = total + jnp.where(lane == 0, 0.0, pltpu.roll(v, 1, 1))
        return v, total - 6.0 * v

    def solve(groups):
        states, shrinks, whiches, limits = [], [], [], []
        for g, cells in enumerate(groups):
            parts = []
            for x, y in cells:
                v, lap = laplace(ext, x, y)
                force = coef[...] * lap
                out[x, y] = force
                parts.append(v + force)
            target = jnp.concatenate(parts, axis=1)
            which = jnp.concatenate([classes[pl.ds(x * ny + y, 1), :] for x, y in cells], axis=1)
            cell_rate = jnp.zeros(which.shape, F32)
            cell_count = jnp.zeros(which.shape, jnp.int32)
            for k in range(nclass):
                cell_rate = jnp.where(which == k, rates[k], cell_rate)
                cell_count = jnp.where(which == k, counts[k], cell_count)
            shrink = 1.0 / (1.0 + cell_rate)
            scaled[g, :, :target.shape[1]] = target * shrink
            states.append(target * cell_rate)
            shrinks.append(shrink)
            whiches.append(which)
            limits.append(cell_count)

        def value(g, state):
            return state * shrinks[g] + scaled[g, :, :state.shape[1]]

        def step(k, states):
            result = []
            for g, state in enumerate(states):
                z = jnp.concatenate([state, jnp.tanh(value(g, state))], axis=0)
                high = z.astype(BF16)
                low = (z - high.astype(F32)).astype(BF16)
                z = jnp.concatenate([high, low], axis=0)
                fixes = jnp.dot(w_high[...], z, preferred_element_type=F32)
                fixes = fixes + jnp.dot(w_low[...], z, preferred_element_type=F32)
                active = jnp.where(k < limits[g], whiches[g], nclass)
                picks = [active == n for n in range(nclass)]
                tiles = []
                for t in range(pad // 8):
                    fix = jnp.zeros((8, state.shape[1]), F32)
                    for n in range(nclass):
                        at = (t * nclass + n) * 8
                        fix = jnp.where(picks[n], fixes[at:at + 8], fix)
                    tiles.append(fix)
                result.append(state + jnp.concatenate(tiles, axis=0))
            return tuple(result)

        states = lax.fori_loop(0, NMAX, step, tuple(states), unroll=NMAX)
        for g, (cells, state) in enumerate(zip(groups, states)):
            end = value(g, state)
            for i, (x, y) in enumerate(cells):
                ext2[x + 1, y + 1] = end[:, i * nz:(i + 1) * nz]

    def pack(cells):
        return [cells[i:i + 2] for i in range(0, len(cells), 2)]

    def solve_all(cells):
        groups = pack(cells)
        for i in range(0, len(groups), SPAN):
            solve(groups[i:i + SPAN])

    for x, y in later:
        load(x, y).wait()
    middle = list(range(1, nx - 1))
    free = [(x, y) for pair in edges[1:] for y in pair for x in middle]
    rim = [(x, y) for y in edges[0] for x in middle]
    now = 2 * SPAN * (len(free) // (2 * SPAN))
    solve_all(free[:now])
    y_arrive(0)
    solve_all(free[now:] + rim)
    per = max(1, SPAN // 2)
    for c in range(0, len(edges), per):
        ys = [y for pair in edges[c:c + per] for y in pair]
        x_arrive(0, ys)
        solve_all([(x, y) for y in ys for x in sides])
        x_start(1, ys)
        if c == 0:
            y_start(1)

    def finish(x, y):
        v, lap = laplace(ext2, x, y)
        out[x, y] = v + 0.5 * (coef[...] * lap - out[x, y])

    for x, y in free:
        finish(x, y)
    y_arrive(1)
    for x, y in rim:
        finish(x, y)
    for pair in edges:
        x_arrive(1, pair)
        for y in pair:
            for x in sides:
                finish(x, y)

    for stage in (0, 1):
        for side in (0, 1):
            @pl.when(has_x[side])
            def _():
                for y in range(ny):
                    x_copy(stage, side, y).wait_send()
            @pl.when(has_y[side])
            def _():
                y_copy(stage, side).wait_send()


def deliver(held, out_hbm, sem):
    spec, nx, ny, _ = out_hbm.shape
    copies = [
        pltpu.make_async_copy(held.at[x, y, pl.ds(0, spec)], out_hbm.at[:, x, y], sem.at[x, y])
        for x in range(nx) for y in range(ny)]
    for copy in copies:
        copy.start()
    for copy in copies:
        copy.wait()


def local(species, diffusion, class_rate, mixing, inverses, newton_counts, cell_class):
    spec, nx, ny, nz = species.shape
    nclass = inverses.shape[0]
    pad = -(-spec // 8) * 8
    anywhere = pl.BlockSpec(memory_space=pl.ANY)
    vmem = pl.BlockSpec(memory_space=pltpu.VMEM)
    held = pl.pallas_call(
        functools.partial(kernel, (spec, nx, ny, nz, nclass)),
        out_shape=pltpu.VMEM((nx, ny, pad, nz), F32),
        in_specs=[anywhere] * 7,
        out_specs=vmem,
        scratch_shapes=[
            pltpu.VMEM((nx + 2, ny + 2, pad, nz), F32),
            pltpu.VMEM((nx + 2, ny + 2, pad, nz), F32),
            pltpu.VMEM((SPAN, pad, 2 * nz), F32),
            pltpu.VMEM((pad, nz), F32),
            pltpu.VMEM((1, spec), F32),
            pltpu.VMEM((spec, spec), F32),
            pltpu.VMEM((spec, nclass, spec), F32),
            pltpu.VMEM((nclass * pad, 128), F32),
            pltpu.VMEM((128, 128), F32),
            pltpu.VMEM((nclass * pad, 4 * pad), BF16),
            pltpu.VMEM((nclass * pad, 4 * pad), BF16),
            pltpu.VMEM((nx * ny, nz), jnp.int32),
            pltpu.SMEM((nclass,), F32),
            pltpu.SMEM((nclass,), jnp.int32),
            pltpu.SemaphoreType.DMA((nx, ny)),
            pltpu.SemaphoreType.DMA((6,)),
            pltpu.SemaphoreType.DMA((2, 2, ny)),
            pltpu.SemaphoreType.DMA((2, 2, ny)),
            pltpu.SemaphoreType.DMA((2, 2)),
            pltpu.SemaphoreType.DMA((2, 2)),
        ],
        compiler_params=pltpu.CompilerParams(
            collective_id=0, has_side_effects=True, vmem_limit_bytes=60 * 1024 * 1024),
    )(
        species, diffusion.reshape(1, spec), class_rate,
        mixing, inverses.transpose(1, 0, 2), newton_counts, cell_class.reshape(nx * ny, nz),
    )
    return pl.pallas_call(
        deliver,
        out_shape=jax.ShapeDtypeStruct(species.shape, F32),
        in_specs=[vmem],
        out_specs=anywhere,
        scratch_shapes=[pltpu.SemaphoreType.DMA((nx, ny))],
    )(pltpu.with_memory_space_constraint(held, pltpu.VMEM))


def solution(mesh):
    in_specs = (P(None, "gx", "gy", None), P(), P(), P(), P(), P(), P("gx", "gy", None))
    out_specs = P(None, "gx", "gy", None)
    return jax.shard_map(local, mesh=mesh, in_specs=in_specs, out_specs=out_specs, check_vma=False)
```

```python
import functools

import jax
import jax.numpy as jnp
from jax import lax
from jax.experimental import pallas as pl
from jax.experimental.pallas import tpu as pltpu
from jax.sharding import PartitionSpec as P

NMAX = 8
SPAN = 4
MESH = pl.DeviceIdType.MESH
F32 = jnp.float32
BF16 = jnp.bfloat16


def pairs_of(n):
    return [tuple(sorted({c, n - 1 - c})) for c in range((n + 1) // 2)]


def kernel(
    dims,
    species_hbm, diffusion_hbm, rate_hbm, mixing_hbm, inverses_hbm, counts_hbm, class_hbm,
    out,
    ext, ext2, scaled, coef, row, mix, inv, stack, square, w_high, w_low, classes, rates, counts,
    load_sem, small_sem, xs_send, xs_recv, ys_send, ys_recv,
):
    spec, nx, ny, nz, nclass = dims
    pad = ext.shape[2]
    real = pl.ds(0, spec)
    gx, gy = lax.axis_index("gx"), lax.axis_index("gy")
    sx, sy = lax.axis_size("gx"), lax.axis_size("gy")
    has_x = (gx > 0, gx < sx - 1)
    has_y = (gy > 0, gy < sy - 1)
    to_x = ((gx - 1, gy), (gx + 1, gy))
    to_y = ((gx, gy - 1), (gx, gy + 1))
    edges = pairs_of(ny)
    order = [y for pair in edges for y in pair]
    slot = {y: at + 1 for at, y in enumerate(order)} | {-1: 0, ny: ny + 1}
    wide = len(edges[0])

    def span(c):
        return pl.ds(slot[edges[c][0]], len(edges[c]))

    sides = sorted({0, nx - 1})
    middle = list(range(1, nx - 1))
    free = [(x, y) for y in order[wide:] for x in middle]
    rim = [(x, y) for y in order[:wide] for x in middle]
    face = [(x, y) for y in order for x in sides]
    corner = wide * len(sides)
    groups = [([(x, y) for y in order], (pl.ds(x + 1, 1), pl.ds(1, ny))) for x in sides]
    groups += [(rim, (pl.ds(2, nx - 2), pl.ds(1, wide))), (free, (pl.ds(2, nx - 2), pl.ds(1 + wide, ny - wide)))]
    groups = [group for group in groups if group[0]]
    kind = {cell: i for i, (cells, _) in enumerate(groups) for cell in cells}
    for x, y in face[:corner] + rim + face[corner:] + free:
        pltpu.make_async_copy(
            species_hbm.at[:, x, y], ext.at[x + 1, slot[y], real], load_sem.at[kind[x, y]]).start()

    def loaded(i):
        box = groups[i][1]
        pltpu.make_async_copy(
            ext2.at[box[0], box[1], real], ext.at[box[0], box[1], real], load_sem.at[i]).wait()

    small = [
        pltpu.make_async_copy(src, dst, small_sem.at[i]) for i, (src, dst) in enumerate((
            (mixing_hbm, mix), (inverses_hbm, inv), (diffusion_hbm, row),
            (rate_hbm, rates), (counts_hbm, counts), (class_hbm, classes)))]
    for copy in small:
        copy.start()

    barrier = pltpu.get_barrier_semaphore()
    for has, to in zip(has_x + has_y, to_x + to_y):
        @pl.when(has)
        def _():
            pl.semaphore_signal(barrier, inc=1, device_id=to, device_id_type=MESH)

    tail = jnp.zeros((pad - spec, nz), F32)
    for x in range(nx + 2):
        for y in range(ny + 2):
            halo = x in (0, nx + 1) or y in (0, ny + 1)
            if x in (0, nx + 1) and y in (0, ny + 1):
                continue
            ext[x, y, pl.ds(spec, pad - spec)] = tail
            if halo:
                ext2[x, y, pl.ds(spec, pad - spec)] = tail
    blank = jnp.zeros((spec, nz), F32)
    for side in (0, 1):
        @pl.when(jnp.logical_not(has_x[side]))
        def _():
            for buf in (ext, ext2):
                for y in range(ny):
                    buf[side * (nx + 1), slot[y], real] = blank
        @pl.when(jnp.logical_not(has_y[side]))
        def _():
            for buf in (ext, ext2):
                for x in range(nx):
                    buf[x + 1, side * (ny + 1), real] = blank

    def x_copy(stage, side, c):
        buf = (ext, ext2)[stage]
        src_row, dst_row = (1, nx + 1) if side == 0 else (nx, 0)
        return pltpu.make_async_remote_copy(
            src_ref=buf.at[src_row, span(c), real], dst_ref=buf.at[dst_row, span(c), real],
            send_sem=xs_send.at[stage, side], recv_sem=xs_recv.at[stage, side, c],
            device_id=to_x[side], device_id_type=MESH)

    def x_face(stage, side):
        buf = (ext, ext2)[stage]
        rows = buf.at[1 if side == 0 else nx, pl.ds(1, ny), real]
        return pltpu.make_async_remote_copy(
            src_ref=rows, dst_ref=rows, send_sem=xs_send.at[stage, side],
            recv_sem=xs_recv.at[stage, side, 0], device_id=to_x[side], device_id_type=MESH)

    def y_copy(stage, side):
        buf = (ext, ext2)[stage]
        src_col, dst_col = (slot[0], ny + 1) if side == 0 else (slot[ny - 1], 0)
        return pltpu.make_async_remote_copy(
            src_ref=buf.at[pl.ds(1, nx), src_col, real],
            dst_ref=buf.at[pl.ds(1, nx), dst_col, real],
            send_sem=ys_send.at[stage, side], recv_sem=ys_recv.at[stage, side],
            device_id=to_y[side], device_id_type=MESH)

    def x_start(stage, cs):
        for side in (0, 1):
            @pl.when(has_x[side])
            def _():
                for c in cs:
                    x_copy(stage, side, c).start()

    def x_arrive(stage, cs):
        for side in (0, 1):
            @pl.when(has_x[side])
            def _():
                for c in cs:
                    x_copy(stage, 1 - side, c).wait_recv()

    def y_start(stage):
        for side in (0, 1):
            @pl.when(has_y[side])
            def _():
                y_copy(stage, side).start()

    def y_arrive(stage):
        for side in (0, 1):
            @pl.when(has_y[side])
            def _():
                y_copy(stage, 1 - side).wait_recv()

    neighbours = sum(has.astype(jnp.int32) for has in has_x + has_y)
    pl.semaphore_wait(barrier, neighbours)
    for i in range(len(groups) - bool(free)):
        loaded(i)
    per = max(1, SPAN // 2)
    batches = [range(len(edges))[c:c + per] for c in range(0, len(edges), per)]
    x_start(0, batches[0][:1])
    y_start(0)
    x_start(0, batches[0][1:])

    for copy in small:
        copy.wait()
    stack[...] = jnp.zeros_like(stack)
    square[...] = jnp.zeros_like(square)
    square[0:1, 0:spec] = row[...]
    line = jnp.broadcast_to(square[0:1, :], square.shape)
    on = lax.broadcasted_iota(jnp.int32, square.shape, 0) == lax.broadcasted_iota(
        jnp.int32, square.shape, 1)
    column = jnp.sum(jnp.where(on, line, 0.0), axis=1, keepdims=True)
    coef[...] = jnp.broadcast_to(column[:pad], coef.shape)
    square[0:spec, 0:spec] = mix[...]
    for k in range(nclass):
        stack[k * pad:k * pad + spec, 0:spec] = inv[:, k, :]
    mixed = jnp.dot(
        stack[...], square[...], precision=lax.Precision.HIGHEST, preferred_element_type=F32)
    spread = lax.broadcasted_iota(jnp.int32, (pad, 128), 1)
    highs, lows = [], []
    for k in range(nclass):
        rate = rates[k]
        own = stack[k * pad:(k + 1) * pad, :] * -(1.0 + rate)
        other = mixed[k * pad:(k + 1) * pad, :] * (rate * (1.0 + rate))
        both = own + pltpu.roll(other, pad, 1)
        high = both.astype(BF16).astype(F32)
        for part, into in ((high, highs), (both - high, lows)):
            turned = pltpu.roll(part, 2 * pad, 1)
            into.append(jnp.concatenate(
                [jnp.where(spread < 2 * pad, part, turned), turned], axis=1))
    for parts, ref in ((highs, w_high), (lows, w_low)):
        ref[...] = jnp.concatenate(
            [parts[k][t * 8:(t + 1) * 8] for t in range(pad // 8) for k in range(nclass)],
            axis=0)[:, :4 * pad].astype(BF16)

    lane = lax.broadcasted_iota(jnp.int32, (pad, nz), 1)

    def laplace(buf, x, y):
        at = slot[y]
        v = buf[x + 1, at]
        total = buf[x + 2, at] + buf[x, at] + buf[x + 1, slot[y + 1]] + buf[x + 1, slot[y - 1]]
        total = total + jnp.where(lane == nz - 1, 0.0, pltpu.roll(v, nz - 1, 1))
        total = total + jnp.where(lane == 0, 0.0, pltpu.roll(v, 1, 1))
        return v, total - 6.0 * v

    def solve(groups):
        states, shrinks, whiches, limits = [], [], [], []
        for g, cells in enumerate(groups):
            parts = []
            for x, y in cells:
                v, lap = laplace(ext, x, y)
                force = coef[...] * lap
                out[x, y] = force
                parts.append(v + force)
            target = jnp.concatenate(parts, axis=1)
            which = jnp.concatenate([classes[pl.ds(x * ny + y, 1), :] for x, y in cells], axis=1)
            cell_rate = jnp.zeros(which.shape, F32)
            cell_count = jnp.zeros(which.shape, jnp.int32)
            for k in range(nclass):
                cell_rate = jnp.where(which == k, rates[k], cell_rate)
                cell_count = jnp.where(which == k, counts[k], cell_count)
            shrink = 1.0 / (1.0 + cell_rate)
            scaled[g, :, :target.shape[1]] = target * shrink
            states.append(target * cell_rate)
            shrinks.append(shrink)
            whiches.append(which)
            limits.append(cell_count)

        def value(g, state):
            return state * shrinks[g] + scaled[g, :, :state.shape[1]]

        def step(k, states):
            result = []
            for g, state in enumerate(states):
                z = jnp.concatenate([state, jnp.tanh(value(g, state))], axis=0)
                high = z.astype(BF16)
                low = (z - high.astype(F32)).astype(BF16)
                z = jnp.concatenate([high, low], axis=0)
                fixes = jnp.dot(w_high[...], z, preferred_element_type=F32)
                fixes = fixes + jnp.dot(w_low[...], z, preferred_element_type=F32)
                active = jnp.where(k < limits[g], whiches[g], nclass)
                picks = [active == n for n in range(nclass)]
                tiles = []
                for t in range(pad // 8):
                    fix = jnp.zeros((8, state.shape[1]), F32)
                    for n in range(nclass):
                        at = (t * nclass + n) * 8
                        fix = jnp.where(picks[n], fixes[at:at + 8], fix)
                    tiles.append(fix)
                result.append(state + jnp.concatenate(tiles, axis=0))
            return tuple(result)

        states = lax.fori_loop(0, NMAX, step, tuple(states), unroll=NMAX)
        for g, (cells, state) in enumerate(zip(groups, states)):
            end = value(g, state)
            for i, (x, y) in enumerate(cells):
                ext2[x + 1, slot[y]] = end[:, i * nz:(i + 1) * nz]

    def pack(cells):
        return [cells[i:i + 2] for i in range(0, len(cells), 2)]

    def solve_all(cells):
        groups = pack(cells)
        for i in range(0, len(groups), SPAN):
            solve(groups[i:i + SPAN])

    if free:
        loaded(len(groups) - 1)
    now = 2 * SPAN * (len(free) // (2 * SPAN))
    solve_all(free[:now])
    for batch in batches[1:]:
        x_start(0, batch)
    y_arrive(0)
    solve_all(free[now:] + rim)
    for i, batch in enumerate(batches):
        x_arrive(0, batch)
        solve_all([(x, y) for c in batch for y in edges[c] for x in sides])
        x_start(1, batch)
        if i == 0:
            y_start(1)

    def finish(x, y):
        v, lap = laplace(ext2, x, y)
        out[x, y] = v + 0.5 * (coef[...] * lap - out[x, y])

    for x, y in free:
        finish(x, y)
    y_arrive(1)
    for x, y in rim:
        finish(x, y)
    for c, pair in enumerate(edges):
        x_arrive(1, [c])
        for y in pair:
            for x in sides:
                finish(x, y)

    for stage in (0, 1):
        for side in (0, 1):
            @pl.when(has_x[side])
            def _():
                x_face(stage, side).wait_send()
            @pl.when(has_y[side])
            def _():
                y_copy(stage, side).wait_send()


def deliver(held, out_hbm, sem):
    spec, nx, ny, _ = out_hbm.shape
    copies = [
        pltpu.make_async_copy(held.at[x, y, pl.ds(0, spec)], out_hbm.at[:, x, y], sem)
        for x in range(nx) for y in range(ny)]
    for copy in copies:
        copy.start()
    every = held.at[:, :, pl.ds(0, spec)]
    pltpu.make_async_copy(every, every, sem).wait()


def local(species, diffusion, class_rate, mixing, inverses, newton_counts, cell_class):
    spec, nx, ny, nz = species.shape
    nclass = inverses.shape[0]
    pad = -(-spec // 8) * 8
    anywhere = pl.BlockSpec(memory_space=pl.ANY)
    vmem = pl.BlockSpec(memory_space=pltpu.VMEM)
    held = pl.pallas_call(
        functools.partial(kernel, (spec, nx, ny, nz, nclass)),
        out_shape=pltpu.VMEM((nx, ny, pad, nz), F32),
        in_specs=[anywhere] * 7,
        out_specs=vmem,
        scratch_shapes=[
            pltpu.VMEM((nx + 2, ny + 2, pad, nz), F32),
            pltpu.VMEM((nx + 2, ny + 2, pad, nz), F32),
            pltpu.VMEM((SPAN, pad, 2 * nz), F32),
            pltpu.VMEM((pad, nz), F32),
            pltpu.VMEM((1, spec), F32),
            pltpu.VMEM((spec, spec), F32),
            pltpu.VMEM((spec, nclass, spec), F32),
            pltpu.VMEM((nclass * pad, 128), F32),
            pltpu.VMEM((128, 128), F32),
            pltpu.VMEM((nclass * pad, 4 * pad), BF16),
            pltpu.VMEM((nclass * pad, 4 * pad), BF16),
            pltpu.VMEM((nx * ny, nz), jnp.int32),
            pltpu.SMEM((nclass,), F32),
            pltpu.SMEM((nclass,), jnp.int32),
            pltpu.SemaphoreType.DMA((4,)),
            pltpu.SemaphoreType.DMA((6,)),
            pltpu.SemaphoreType.DMA((2, 2)),
            pltpu.SemaphoreType.DMA((2, 2, (ny + 1) // 2)),
            pltpu.SemaphoreType.DMA((2, 2)),
            pltpu.SemaphoreType.DMA((2, 2)),
        ],
        compiler_params=pltpu.CompilerParams(
            collective_id=0, has_side_effects=True, vmem_limit_bytes=60 * 1024 * 1024),
    )(
        species, diffusion.reshape(1, spec), class_rate,
        mixing, inverses.transpose(1, 0, 2), newton_counts, cell_class.reshape(nx * ny, nz),
    )
    return pl.pallas_call(
        deliver,
        out_shape=jax.ShapeDtypeStruct(species.shape, F32),
        in_specs=[vmem],
        out_specs=anywhere,
        scratch_shapes=[pltpu.SemaphoreType.DMA(())],
    )(pltpu.with_memory_space_constraint(held, pltpu.VMEM))


def solution(mesh):
    in_specs = (P(None, "gx", "gy", None), P(), P(), P(), P(), P(), P("gx", "gy", None))
    out_specs = P(None, "gx", "gy", None)
    return jax.shard_map(local, mesh=mesh, in_specs=in_specs, out_specs=out_specs, check_vma=False)
```

```python
import functools

import jax
import jax.numpy as jnp
from jax import lax
from jax.experimental import pallas as pl
from jax.experimental.pallas import tpu as pltpu
from jax.sharding import PartitionSpec as P

NMAX = 8
SPAN = 6
WHEN = 3
MESH = pl.DeviceIdType.MESH
F32 = jnp.float32
BF16 = jnp.bfloat16


def pairs_of(n):
    return [tuple(sorted({c, n - 1 - c})) for c in range((n + 1) // 2)]


def kernel(
    dims,
    species_hbm, diffusion_hbm, rate_hbm, mixing_hbm, inverses_hbm, counts_hbm, class_hbm,
    out,
    ext, ext2, scaled, coef, row, mix, inv, stack, square, w_high, w_low, classes, rates, counts,
    load_sem, small_sem, xs_send, xs_recv, ys_send, ys_recv,
):
    spec, nx, ny, nz, nclass = dims
    pad = ext.shape[2]
    real = pl.ds(0, spec)
    gx, gy = lax.axis_index("gx"), lax.axis_index("gy")
    sx, sy = lax.axis_size("gx"), lax.axis_size("gy")
    has_x = (gx > 0, gx < sx - 1)
    has_y = (gy > 0, gy < sy - 1)
    to_x = ((gx - 1, gy), (gx + 1, gy))
    to_y = ((gx, gy - 1), (gx, gy + 1))
    edges = pairs_of(ny)
    order = [y for pair in edges for y in pair]
    slot = {y: at + 1 for at, y in enumerate(order)} | {-1: 0, ny: ny + 1}
    wide = len(edges[0])

    pieces = ([pl.ds(1, ny)], [pl.ds(slot[pair[0]], len(pair)) for pair in edges])
    sides = sorted({0, nx - 1})
    middle = list(range(1, nx - 1))
    free = [(x, y) for y in order[wide:] for x in middle]
    rim = [(x, y) for y in order[:wide] for x in middle]
    face = [(x, y) for y in order for x in sides]
    corner = wide * len(sides)
    groups = [([(x, y) for y in order], (pl.ds(x + 1, 1), pl.ds(1, ny))) for x in sides]
    groups += [(rim, (pl.ds(2, nx - 2), pl.ds(1, wide))), (free, (pl.ds(2, nx - 2), pl.ds(1 + wide, ny - wide)))]
    groups = [group for group in groups if group[0]]
    kind = {cell: i for i, (cells, _) in enumerate(groups) for cell in cells}
    for x, y in face[:corner] + rim + face[corner:] + free:
        pltpu.make_async_copy(
            species_hbm.at[:, x, y], ext.at[x + 1, slot[y], real], load_sem.at[kind[x, y]]).start()

    def loaded(i):
        box = groups[i][1]
        pltpu.make_async_copy(
            ext2.at[box[0], box[1], real], ext.at[box[0], box[1], real], load_sem.at[i]).wait()

    small = [
        pltpu.make_async_copy(src, dst, small_sem.at[i]) for i, (src, dst) in enumerate((
            (mixing_hbm, mix), (inverses_hbm, inv), (diffusion_hbm, row),
            (rate_hbm, rates), (counts_hbm, counts), (class_hbm, classes)))]
    for copy in small:
        copy.start()

    barrier = pltpu.get_barrier_semaphore()
    for has, to in zip(has_x + has_y, to_x + to_y):
        @pl.when(has)
        def _():
            pl.semaphore_signal(barrier, inc=1, device_id=to, device_id_type=MESH)

    tail = jnp.zeros((pad - spec, nz), F32)
    for x in range(nx + 2):
        for y in range(ny + 2):
            halo = x in (0, nx + 1) or y in (0, ny + 1)
            if x in (0, nx + 1) and y in (0, ny + 1):
                continue
            ext[x, y, pl.ds(spec, pad - spec)] = tail
            if halo:
                ext2[x, y, pl.ds(spec, pad - spec)] = tail
    blank = jnp.zeros((spec, nz), F32)
    for side in (0, 1):
        @pl.when(jnp.logical_not(has_x[side]))
        def _():
            for buf in (ext, ext2):
                for y in range(ny):
                    buf[side * (nx + 1), slot[y], real] = blank
        @pl.when(jnp.logical_not(has_y[side]))
        def _():
            for buf in (ext, ext2):
                for x in range(nx):
                    buf[x + 1, side * (ny + 1), real] = blank

    def x_copy(stage, side, c):
        buf = (ext, ext2)[stage]
        src_row, dst_row = (1, nx + 1) if side == 0 else (nx, 0)
        return pltpu.make_async_remote_copy(
            src_ref=buf.at[src_row, pieces[stage][c], real],
            dst_ref=buf.at[dst_row, pieces[stage][c], real],
            send_sem=xs_send.at[stage, side], recv_sem=xs_recv.at[side, stage + c],
            device_id=to_x[side], device_id_type=MESH)

    def x_face(stage, side):
        buf = (ext, ext2)[stage]
        rows = buf.at[1 if side == 0 else nx, pl.ds(1, ny), real]
        return pltpu.make_async_remote_copy(
            src_ref=rows, dst_ref=rows, send_sem=xs_send.at[stage, side],
            recv_sem=xs_recv.at[side, 0], device_id=to_x[side], device_id_type=MESH)

    def y_copy(stage, side):
        buf = (ext, ext2)[stage]
        src_col, dst_col = (slot[0], ny + 1) if side == 0 else (slot[ny - 1], 0)
        return pltpu.make_async_remote_copy(
            src_ref=buf.at[pl.ds(1, nx), src_col, real],
            dst_ref=buf.at[pl.ds(1, nx), dst_col, real],
            send_sem=ys_send.at[stage, side], recv_sem=ys_recv.at[stage, side],
            device_id=to_y[side], device_id_type=MESH)

    even = gx % 2 == 0
    near = (jnp.logical_not(even), even)

    def facing(close):
        for side in (0, 1):
            mine = near[side] if close else jnp.logical_not(near[side])
            yield side, jnp.logical_and(has_x[side], mine)

    def x_start(stage, close):
        for side, there in facing(close):
            @pl.when(there)
            def _():
                for c in range(len(pieces[stage])):
                    x_copy(stage, side, c).start()

    def x_arrive(stage, close, c):
        for side, there in facing(close):
            @pl.when(there)
            def _():
                x_copy(stage, 1 - side, c).wait_recv()

    def y_start(stage):
        for side in (0, 1):
            @pl.when(has_y[side])
            def _():
                y_copy(stage, side).start()

    def y_arrive(stage):
        for side in (0, 1):
            @pl.when(has_y[side])
            def _():
                y_copy(stage, 1 - side).wait_recv()

    neighbours = sum(has.astype(jnp.int32) for has in has_x + has_y)
    pl.semaphore_wait(barrier, neighbours)
    for i in range(len(groups) - bool(free)):
        loaded(i)
    x_start(0, True)
    y_start(0)

    for copy in small:
        copy.wait()
    stack[...] = jnp.zeros_like(stack)
    square[...] = jnp.zeros_like(square)
    square[0:1, 0:spec] = row[...]
    line = jnp.broadcast_to(square[0:1, :], square.shape)
    on = lax.broadcasted_iota(jnp.int32, square.shape, 0) == lax.broadcasted_iota(
        jnp.int32, square.shape, 1)
    column = jnp.sum(jnp.where(on, line, 0.0), axis=1, keepdims=True)
    coef[...] = jnp.broadcast_to(column[:pad], coef.shape)
    square[0:spec, 0:spec] = mix[...]
    for k in range(nclass):
        stack[k * pad:k * pad + spec, 0:spec] = inv[:, k, :]
    mixed = jnp.dot(
        stack[...], square[...], precision=lax.Precision.HIGHEST, preferred_element_type=F32)
    spread = lax.broadcasted_iota(jnp.int32, (pad, 128), 1)
    highs, lows = [], []
    for k in range(nclass):
        rate = rates[k]
        own = stack[k * pad:(k + 1) * pad, :] * -(1.0 + rate)
        other = mixed[k * pad:(k + 1) * pad, :] * (rate * (1.0 + rate))
        both = own + pltpu.roll(other, pad, 1)
        high = both.astype(BF16).astype(F32)
        for part, into in ((high, highs), (both - high, lows)):
            turned = pltpu.roll(part, 2 * pad, 1)
            into.append(jnp.concatenate(
                [jnp.where(spread < 2 * pad, part, turned), turned], axis=1))
    for parts, ref in ((highs, w_high), (lows, w_low)):
        ref[...] = jnp.concatenate(
            [parts[k][t * 8:(t + 1) * 8] for t in range(pad // 8) for k in range(nclass)],
            axis=0)[:, :4 * pad].astype(BF16)

    lane = lax.broadcasted_iota(jnp.int32, (pad, nz), 1)

    def laplace(buf, x, y):
        at = slot[y]
        v = buf[x + 1, at]
        total = buf[x + 2, at] + buf[x, at] + buf[x + 1, slot[y + 1]] + buf[x + 1, slot[y - 1]]
        total = total + jnp.where(lane == nz - 1, 0.0, pltpu.roll(v, nz - 1, 1))
        total = total + jnp.where(lane == 0, 0.0, pltpu.roll(v, 1, 1))
        return v, total - 6.0 * v

    def solve(groups, hook):
        states, shrinks, whiches, limits = [], [], [], []
        for g, cells in enumerate(groups):
            parts = []
            for x, y in cells:
                v, lap = laplace(ext, x, y)
                force = coef[...] * lap
                out[x, y] = force
                parts.append(v + force)
            target = jnp.concatenate(parts, axis=1)
            which = jnp.concatenate([classes[pl.ds(x * ny + y, 1), :] for x, y in cells], axis=1)
            cell_rate = jnp.zeros(which.shape, F32)
            cell_count = jnp.zeros(which.shape, jnp.int32)
            for k in range(nclass):
                cell_rate = jnp.where(which == k, rates[k], cell_rate)
                cell_count = jnp.where(which == k, counts[k], cell_count)
            shrink = 1.0 / (1.0 + cell_rate)
            scaled[g, :, :target.shape[1]] = target * shrink
            states.append(target * cell_rate)
            shrinks.append(shrink)
            whiches.append(which)
            limits.append(cell_count)

        def value(g, state):
            return state * shrinks[g] + scaled[g, :, :state.shape[1]]

        def step(k, states):
            result = []
            for g, state in enumerate(states):
                z = jnp.concatenate([state, jnp.tanh(value(g, state))], axis=0)
                high = z.astype(BF16)
                low = (z - high.astype(F32)).astype(BF16)
                z = jnp.concatenate([high, low], axis=0)
                fixes = jnp.dot(w_high[...], z, preferred_element_type=F32)
                fixes = fixes + jnp.dot(w_low[...], z, preferred_element_type=F32)
                active = jnp.where(k < limits[g], whiches[g], nclass)
                picks = [active == n for n in range(nclass)]
                tiles = []
                for t in range(pad // 8):
                    fix = jnp.zeros((8, state.shape[1]), F32)
                    for n in range(nclass):
                        at = (t * nclass + n) * 8
                        fix = jnp.where(picks[n], fixes[at:at + 8], fix)
                    tiles.append(fix)
                result.append(state + jnp.concatenate(tiles, axis=0))
            return tuple(result)

        states, part = tuple(states), NMAX if hook is None else WHEN
        states = lax.fori_loop(0, part, step, states, unroll=part)
        if hook is not None:
            hook()
            states = lax.fori_loop(part, NMAX, step, states, unroll=NMAX - part)
        for g, (cells, state) in enumerate(zip(groups, states)):
            end = value(g, state)
            for i, (x, y) in enumerate(cells):
                ext2[x + 1, slot[y]] = end[:, i * nz:(i + 1) * nz]

    def pack(cells):
        return [cells[i:i + 2] for i in range(0, len(cells), 2)]

    def solve_all(cells, hook=None):
        groups = pack(cells)
        for i in range(0, len(groups), SPAN):
            solve(groups[i:i + SPAN], hook if i == 0 else None)

    if free:
        loaded(len(groups) - 1)
    near_x = (1 - gx % 2) * (nx - 1)
    far_x = nx - 1 - near_x
    solve_all(free)
    y_arrive(0)
    solve_all(rim, lambda: x_start(0, False))
    x_arrive(0, True, 0)
    solve_all([(near_x, y) for y in order])
    x_start(1, True)
    x_arrive(0, False, 0)
    solve_all([(far_x, y) for y in order])
    x_start(1, False)
    y_start(1)

    def finish(x, y):
        v, lap = laplace(ext2, x, y)
        out[x, y] = v + 0.5 * (coef[...] * lap - out[x, y])

    for x, y in free:
        finish(x, y)
    y_arrive(1)
    for x, y in rim:
        finish(x, y)
    for close, x in ((True, near_x), (False, far_x)):
        for c, pair in enumerate(edges):
            x_arrive(1, close, c)
            for y in pair:
                finish(x, y)

    for stage in (0, 1):
        for close in (True, False):
            for side, there in facing(close):
                @pl.when(there)
                def _():
                    x_face(stage, side).wait_send()
        for side in (0, 1):
            @pl.when(has_y[side])
            def _():
                y_copy(stage, side).wait_send()


def deliver(held, out_hbm, sem):
    spec, nx, ny, _ = out_hbm.shape
    copies = [
        pltpu.make_async_copy(held.at[x, y, pl.ds(0, spec)], out_hbm.at[:, x, y], sem)
        for x in range(nx) for y in range(ny)]
    for copy in copies:
        copy.start()
    every = held.at[:, :, pl.ds(0, spec)]
    pltpu.make_async_copy(every, every, sem).wait()


def local(species, diffusion, class_rate, mixing, inverses, newton_counts, cell_class):
    spec, nx, ny, nz = species.shape
    nclass = inverses.shape[0]
    pad = -(-spec // 8) * 8
    anywhere = pl.BlockSpec(memory_space=pl.ANY)
    vmem = pl.BlockSpec(memory_space=pltpu.VMEM)
    held = pl.pallas_call(
        functools.partial(kernel, (spec, nx, ny, nz, nclass)),
        out_shape=pltpu.VMEM((nx, ny, pad, nz), F32),
        in_specs=[anywhere] * 7,
        out_specs=vmem,
        scratch_shapes=[
            pltpu.VMEM((nx + 2, ny + 2, pad, nz), F32),
            pltpu.VMEM((nx + 2, ny + 2, pad, nz), F32),
            pltpu.VMEM((SPAN, pad, 2 * nz), F32),
            pltpu.VMEM((pad, nz), F32),
            pltpu.VMEM((1, spec), F32),
            pltpu.VMEM((spec, spec), F32),
            pltpu.VMEM((spec, nclass, spec), F32),
            pltpu.VMEM((nclass * pad, 128), F32),
            pltpu.VMEM((128, 128), F32),
            pltpu.VMEM((nclass * pad, 4 * pad), BF16),
            pltpu.VMEM((nclass * pad, 4 * pad), BF16),
            pltpu.VMEM((nx * ny, nz), jnp.int32),
            pltpu.SMEM((nclass,), F32),
            pltpu.SMEM((nclass,), jnp.int32),
            pltpu.SemaphoreType.DMA((4,)),
            pltpu.SemaphoreType.DMA((6,)),
            pltpu.SemaphoreType.DMA((2, 2)),
            pltpu.SemaphoreType.DMA((2, 1 + (ny + 1) // 2)),
            pltpu.SemaphoreType.DMA((2, 2)),
            pltpu.SemaphoreType.DMA((2, 2)),
        ],
        compiler_params=pltpu.CompilerParams(
            collective_id=0, has_side_effects=True, vmem_limit_bytes=60 * 1024 * 1024),
    )(
        species, diffusion.reshape(1, spec), class_rate,
        mixing, inverses.transpose(1, 0, 2), newton_counts, cell_class.reshape(nx * ny, nz),
    )
    return pl.pallas_call(
        deliver,
        out_shape=jax.ShapeDtypeStruct(species.shape, F32),
        in_specs=[vmem],
        out_specs=anywhere,
        scratch_shapes=[pltpu.SemaphoreType.DMA(())],
    )(pltpu.with_memory_space_constraint(held, pltpu.VMEM))


def solution(mesh):
    in_specs = (P(None, "gx", "gy", None), P(), P(), P(), P(), P(), P("gx", "gy", None))
    out_specs = P(None, "gx", "gy", None)
    return jax.shard_map(local, mesh=mesh, in_specs=in_specs, out_specs=out_specs, check_vma=False)
```

```python
import functools

import jax
import jax.numpy as jnp
from jax import lax
from jax.experimental import pallas as pl
from jax.experimental.pallas import tpu as pltpu
from jax.sharding import PartitionSpec as P

NMAX = 8
SPAN = 4
MESH = pl.DeviceIdType.MESH
F32 = jnp.float32
BF16 = jnp.bfloat16


def pairs_of(n):
    return [tuple(sorted({c, n - 1 - c})) for c in range((n + 1) // 2)]


def kernel(
    dims,
    species_hbm, diffusion_hbm, rate_hbm, mixing_hbm, inverses_hbm, counts_hbm, class_hbm,
    out,
    ext, ext2, scaled, coef, row, mix, inv, stack, square, w_high, w_low, classes, rates, counts,
    load_sem, small_sem, xs_send, xs_recv, ys_send, ys_recv,
):
    spec, nx, ny, nz, nclass = dims
    pad = ext.shape[2]
    real = pl.ds(0, spec)
    gx, gy = lax.axis_index("gx"), lax.axis_index("gy")
    sx, sy = lax.axis_size("gx"), lax.axis_size("gy")
    has_x = (gx > 0, gx < sx - 1)
    has_y = (gy > 0, gy < sy - 1)
    to_x = ((gx - 1, gy), (gx + 1, gy))
    to_y = ((gx, gy - 1), (gx, gy + 1))
    barrier = pltpu.get_barrier_semaphore()
    for has, to in zip(has_x + has_y, to_x + to_y):
        @pl.when(has)
        def _():
            pl.semaphore_signal(barrier, inc=1, device_id=to, device_id_type=MESH)

    edges = pairs_of(ny)
    order = [y for pair in edges for y in pair]
    slot = {y: at + 1 for at, y in enumerate(order)} | {-1: 0, ny: ny + 1}
    wide = len(edges[0])

    cut = (len(edges) + 1) // 2
    halves = [edges[:cut], edges[cut:]] if edges[cut:] else [edges]
    columns = [[y for pair in half for y in pair] for half in halves]
    pieces = [pl.ds(slot[half[0]], len(half)) for half in columns]
    sides = sorted({0, nx - 1})
    middle = list(range(1, nx - 1))
    free = [(x, y) for y in order[wide:] for x in middle]
    rim = [(x, y) for y in order[:wide] for x in middle]
    face = [(x, y) for y in order for x in sides]
    corner = wide * len(sides)
    groups = [([(x, y) for y in order], (pl.ds(x + 1, 1), pl.ds(1, ny))) for x in sides]
    groups += [(rim, (pl.ds(2, nx - 2), pl.ds(1, wide))), (free, (pl.ds(2, nx - 2), pl.ds(1 + wide, ny - wide)))]
    groups = [group for group in groups if group[0]]
    kind = {cell: i for i, (cells, _) in enumerate(groups) for cell in cells}
    for x, y in face[:corner] + rim + face[corner:] + free:
        pltpu.make_async_copy(
            species_hbm.at[:, x, y], ext.at[x + 1, slot[y], real], load_sem.at[kind[x, y]]).start()

    def loaded(i):
        box = groups[i][1]
        pltpu.make_async_copy(
            ext2.at[box[0], box[1], real], ext.at[box[0], box[1], real], load_sem.at[i]).wait()

    small = [
        pltpu.make_async_copy(src, dst, small_sem.at[i]) for i, (src, dst) in enumerate((
            (mixing_hbm, mix), (inverses_hbm, inv), (diffusion_hbm, row),
            (rate_hbm, rates), (counts_hbm, counts), (class_hbm, classes)))]
    for copy in small:
        copy.start()

    tail = jnp.zeros((pad - spec, nz), F32)
    for x in range(nx + 2):
        for y in range(ny + 2):
            halo = x in (0, nx + 1) or y in (0, ny + 1)
            if x in (0, nx + 1) and y in (0, ny + 1):
                continue
            ext[x, y, pl.ds(spec, pad - spec)] = tail
            if halo:
                ext2[x, y, pl.ds(spec, pad - spec)] = tail
    blank = jnp.zeros((spec, nz), F32)
    for side in (0, 1):
        @pl.when(jnp.logical_not(has_x[side]))
        def _():
            for buf in (ext, ext2):
                for y in range(ny):
                    buf[side * (nx + 1), slot[y], real] = blank
        @pl.when(jnp.logical_not(has_y[side]))
        def _():
            for buf in (ext, ext2):
                for x in range(nx):
                    buf[x + 1, side * (ny + 1), real] = blank

    def x_copy(stage, side, c):
        buf = (ext, ext2)[stage]
        src_row, dst_row = (1, nx + 1) if side == 0 else (nx, 0)
        return pltpu.make_async_remote_copy(
            src_ref=buf.at[src_row, pieces[c], real],
            dst_ref=buf.at[dst_row, pieces[c], real],
            send_sem=xs_send.at[stage, side], recv_sem=xs_recv.at[side, stage * len(halves) + c],
            device_id=to_x[side], device_id_type=MESH)

    def x_face(stage, side):
        buf = (ext, ext2)[stage]
        rows = buf.at[1 if side == 0 else nx, pl.ds(1, ny), real]
        return pltpu.make_async_remote_copy(
            src_ref=rows, dst_ref=rows, send_sem=xs_send.at[stage, side],
            recv_sem=xs_recv.at[side, 0], device_id=to_x[side], device_id_type=MESH)

    def y_copy(stage, side):
        buf = (ext, ext2)[stage]
        src_col, dst_col = (slot[0], ny + 1) if side == 0 else (slot[ny - 1], 0)
        return pltpu.make_async_remote_copy(
            src_ref=buf.at[pl.ds(1, nx), src_col, real],
            dst_ref=buf.at[pl.ds(1, nx), dst_col, real],
            send_sem=ys_send.at[stage, side], recv_sem=ys_recv.at[stage, side],
            device_id=to_y[side], device_id_type=MESH)

    even = gx % 2 == 0
    near = (jnp.logical_not(even), even)

    def facing(close):
        for side in (0, 1):
            mine = near[side] if close else jnp.logical_not(near[side])
            yield side, jnp.logical_and(has_x[side], mine)

    def x_start(stage, close, cs=None):
        for side, there in facing(close):
            @pl.when(there)
            def _():
                for c in range(len(pieces)) if cs is None else cs:
                    x_copy(stage, side, c).start()

    def x_arrive(stage, close, c):
        for side, there in facing(close):
            @pl.when(there)
            def _():
                x_copy(stage, 1 - side, c).wait_recv()

    def y_start(stage):
        for side in (0, 1):
            @pl.when(has_y[side])
            def _():
                y_copy(stage, side).start()

    def y_arrive(stage):
        for side in (0, 1):
            @pl.when(has_y[side])
            def _():
                y_copy(stage, 1 - side).wait_recv()

    neighbours = sum(has.astype(jnp.int32) for has in has_x + has_y)
    pl.semaphore_wait(barrier, neighbours)
    for i in range(len(groups) - bool(free)):
        loaded(i)
    x_start(0, True)
    y_start(0)

    for copy in small:
        copy.wait()
    stack[...] = jnp.zeros_like(stack)
    square[...] = jnp.zeros_like(square)
    square[0:1, 0:spec] = row[...]
    line = jnp.broadcast_to(square[0:1, :], square.shape)
    on = lax.broadcasted_iota(jnp.int32, square.shape, 0) == lax.broadcasted_iota(
        jnp.int32, square.shape, 1)
    column = jnp.sum(jnp.where(on, line, 0.0), axis=1, keepdims=True)
    coef[...] = jnp.broadcast_to(column[:pad], coef.shape)
    square[0:spec, 0:spec] = mix[...]
    for k in range(nclass):
        stack[k * pad:k * pad + spec, 0:spec] = inv[:, k, :]
    mixed = jnp.dot(
        stack[...], square[...], precision=lax.Precision.HIGHEST, preferred_element_type=F32)
    spread = lax.broadcasted_iota(jnp.int32, (pad, 128), 1)
    highs, lows = [], []
    for k in range(nclass):
        rate = rates[k]
        own = stack[k * pad:(k + 1) * pad, :] * -(1.0 + rate)
        other = mixed[k * pad:(k + 1) * pad, :] * (rate * (1.0 + rate))
        both = own + pltpu.roll(other, pad, 1)
        high = both.astype(BF16).astype(F32)
        for part, into in ((high, highs), (both - high, lows)):
            turned = pltpu.roll(part, 2 * pad, 1)
            into.append(jnp.concatenate(
                [jnp.where(spread < 2 * pad, part, turned), turned], axis=1))
    for parts, ref in ((highs, w_high), (lows, w_low)):
        ref[...] = jnp.concatenate(
            [parts[k][t * 8:(t + 1) * 8] for t in range(pad // 8) for k in range(nclass)],
            axis=0)[:, :4 * pad].astype(BF16)

    lane = lax.broadcasted_iota(jnp.int32, (pad, nz), 1)

    def laplace(buf, x, y):
        at = slot[y]
        v = buf[x + 1, at]
        total = buf[x + 2, at] + buf[x, at] + buf[x + 1, slot[y + 1]] + buf[x + 1, slot[y - 1]]
        total = total + jnp.where(lane == nz - 1, 0.0, pltpu.roll(v, nz - 1, 1))
        total = total + jnp.where(lane == 0, 0.0, pltpu.roll(v, 1, 1))
        return v, total - 6.0 * v

    def solve(groups):
        states, shrinks, whiches, limits = [], [], [], []
        for g, cells in enumerate(groups):
            parts = []
            for x, y in cells:
                v, lap = laplace(ext, x, y)
                force = coef[...] * lap
                out[x, y] = force
                parts.append(v + force)
            target = jnp.concatenate(parts, axis=1)
            which = jnp.concatenate([classes[pl.ds(x * ny + y, 1), :] for x, y in cells], axis=1)
            cell_rate = jnp.zeros(which.shape, F32)
            cell_count = jnp.zeros(which.shape, jnp.int32)
            for k in range(nclass):
                cell_rate = jnp.where(which == k, rates[k], cell_rate)
                cell_count = jnp.where(which == k, counts[k], cell_count)
            shrink = 1.0 / (1.0 + cell_rate)
            scaled[g, :, :target.shape[1]] = target * shrink
            states.append(target * cell_rate)
            shrinks.append(shrink)
            whiches.append(which)
            limits.append(cell_count)

        def value(g, state):
            return state * shrinks[g] + scaled[g, :, :state.shape[1]]

        def step(k, states):
            result = []
            for g, state in enumerate(states):
                z = jnp.concatenate([state, jnp.tanh(value(g, state))], axis=0)
                high = z.astype(BF16)
                low = (z - high.astype(F32)).astype(BF16)
                z = jnp.concatenate([high, low], axis=0)
                fixes = jnp.dot(w_high[...], z, preferred_element_type=F32)
                fixes = fixes + jnp.dot(w_low[...], z, preferred_element_type=F32)
                active = jnp.where(k < limits[g], whiches[g], nclass)
                picks = [active == n for n in range(nclass)]
                tiles = []
                for t in range(pad // 8):
                    fix = jnp.zeros((8, state.shape[1]), F32)
                    for n in range(nclass):
                        at = (t * nclass + n) * 8
                        fix = jnp.where(picks[n], fixes[at:at + 8], fix)
                    tiles.append(fix)
                result.append(state + jnp.concatenate(tiles, axis=0))
            return tuple(result)

        states = lax.fori_loop(0, NMAX, step, tuple(states), unroll=NMAX)
        for g, (cells, state) in enumerate(zip(groups, states)):
            end = value(g, state)
            for i, (x, y) in enumerate(cells):
                ext2[x + 1, slot[y]] = end[:, i * nz:(i + 1) * nz]

    def pack(cells):
        return [cells[i:i + 2] for i in range(0, len(cells), 2)]

    def solve_all(cells):
        groups = pack(cells)
        for i in range(0, len(groups), SPAN):
            solve(groups[i:i + SPAN])

    if free:
        loaded(len(groups) - 1)
    near_x = (1 - gx % 2) * (nx - 1)
    far_x = nx - 1 - near_x
    first = 2 * (2 * len(free) // 6)
    solve_all(free[:first])
    solve_all(free[first:])
    x_start(0, False, [0])
    y_arrive(0)
    for h in range(len(halves)):
        x_arrive(0, True, h)
    x_start(0, False, range(1, len(halves)))
    solve_all([(near_x, y) for y in order])
    x_start(1, True)
    for h, half in enumerate(columns):
        x_arrive(0, False, h)
        last = h == len(halves) - 1
        solve_all([(far_x, y) for y in half] + (rim if last else []))
        x_start(1, False, [h])
    y_start(1)

    def finish(x, y):
        v, lap = laplace(ext2, x, y)
        out[x, y] = v + 0.5 * (coef[...] * lap - out[x, y])

    def inside(x, y):
        at = slot[y]
        v = ext2[x + 1, at]
        total = ext2[jnp.where(x == 0, 2, nx - 1), at]
        total = total + ext2[x + 1, slot[y + 1]] + ext2[x + 1, slot[y - 1]]
        total = total + jnp.where(lane == nz - 1, 0.0, pltpu.roll(v, nz - 1, 1))
        total = total + jnp.where(lane == 0, 0.0, pltpu.roll(v, 1, 1))
        out[x, y] = v + 0.5 * (coef[...] * (total - 6.0 * v) - out[x, y])

    def across(x, y):
        out[x, y] = out[x, y] + 0.5 * coef[...] * ext2[jnp.where(x == 0, 0, nx + 1), slot[y]]

    for x, y in free:
        finish(x, y)
    for y in order[wide:]:
        for x in (near_x, far_x):
            inside(x, y)
    y_arrive(1)
    for x, y in rim:
        finish(x, y)
    for y in order[:wide]:
        for x in (near_x, far_x):
            inside(x, y)
    for close, x in ((False, far_x), (True, near_x)):
        for h, half in enumerate(columns):
            x_arrive(1, close, h)
            for y in half:
                across(x, y)

    for stage in (0, 1):
        for close in (True, False):
            for side, there in facing(close):
                @pl.when(there)
                def _():
                    x_face(stage, side).wait_send()
        for side in (0, 1):
            @pl.when(has_y[side])
            def _():
                y_copy(stage, side).wait_send()


def deliver(held, out_hbm, sem):
    spec, nx, ny, _ = out_hbm.shape
    copies = [
        pltpu.make_async_copy(held.at[x, y, pl.ds(0, spec)], out_hbm.at[:, x, y], sem)
        for x in range(nx) for y in range(ny)]
    for copy in copies:
        copy.start()
    every = held.at[:, :, pl.ds(0, spec)]
    pltpu.make_async_copy(every, every, sem).wait()


def local(species, diffusion, class_rate, mixing, inverses, newton_counts, cell_class):
    spec, nx, ny, nz = species.shape
    nclass = inverses.shape[0]
    pad = -(-spec // 8) * 8
    anywhere = pl.BlockSpec(memory_space=pl.ANY)
    vmem = pl.BlockSpec(memory_space=pltpu.VMEM)
    held = pl.pallas_call(
        functools.partial(kernel, (spec, nx, ny, nz, nclass)),
        out_shape=pltpu.VMEM((nx, ny, pad, nz), F32),
        in_specs=[anywhere] * 7,
        out_specs=vmem,
        scratch_shapes=[
            pltpu.VMEM((nx + 2, ny + 2, pad, nz), F32),
            pltpu.VMEM((nx + 2, ny + 2, pad, nz), F32),
            pltpu.VMEM((SPAN, pad, 2 * nz), F32),
            pltpu.VMEM((pad, nz), F32),
            pltpu.VMEM((1, spec), F32),
            pltpu.VMEM((spec, spec), F32),
            pltpu.VMEM((spec, nclass, spec), F32),
            pltpu.VMEM((nclass * pad, 128), F32),
            pltpu.VMEM((128, 128), F32),
            pltpu.VMEM((nclass * pad, 4 * pad), BF16),
            pltpu.VMEM((nclass * pad, 4 * pad), BF16),
            pltpu.VMEM((nx * ny, nz), jnp.int32),
            pltpu.SMEM((nclass,), F32),
            pltpu.SMEM((nclass,), jnp.int32),
            pltpu.SemaphoreType.DMA((4,)),
            pltpu.SemaphoreType.DMA((6,)),
            pltpu.SemaphoreType.DMA((2, 2)),
            pltpu.SemaphoreType.DMA((2, 4)),
            pltpu.SemaphoreType.DMA((2, 2)),
            pltpu.SemaphoreType.DMA((2, 2)),
        ],
        compiler_params=pltpu.CompilerParams(
            collective_id=0, has_side_effects=True, vmem_limit_bytes=60 * 1024 * 1024),
    )(
        species, diffusion.reshape(1, spec), class_rate,
        mixing, inverses.transpose(1, 0, 2), newton_counts, cell_class.reshape(nx * ny, nz),
    )
    return pl.pallas_call(
        deliver,
        out_shape=jax.ShapeDtypeStruct(species.shape, F32),
        in_specs=[vmem],
        out_specs=anywhere,
        scratch_shapes=[pltpu.SemaphoreType.DMA(())],
    )(pltpu.with_memory_space_constraint(held, pltpu.VMEM))


def solution(mesh):
    in_specs = (P(None, "gx", "gy", None), P(), P(), P(), P(), P(), P("gx", "gy", None))
    out_specs = P(None, "gx", "gy", None)
    return jax.shard_map(local, mesh=mesh, in_specs=in_specs, out_specs=out_specs, check_vma=False)
```

```python
import functools

import jax
import jax.numpy as jnp
from jax import lax
from jax.experimental import pallas as pl
from jax.experimental.pallas import tpu as pltpu
from jax.sharding import PartitionSpec as P

NMAX = 8
SPAN = 4
MESH = pl.DeviceIdType.MESH
F32 = jnp.float32
BF16 = jnp.bfloat16


def pairs_of(n):
    return [tuple(sorted({c, n - 1 - c})) for c in range((n + 1) // 2)]


def kernel(
    dims,
    species_hbm, diffusion_hbm, rate_hbm, mixing_hbm, inverses_hbm, counts_hbm, class_hbm,
    out,
    ext, ext2, scaled, coef, row, mix, inv, stack, square, w_high, w_low, classes, rates, counts,
    load_sem, small_sem, xs_send, xs_recv, ys_send, ys_recv,
):
    spec, nx, ny, nz, nclass = dims
    pad = ext.shape[2]
    real = pl.ds(0, spec)
    gx, gy = lax.axis_index("gx"), lax.axis_index("gy")
    sx, sy = lax.axis_size("gx"), lax.axis_size("gy")
    has_x = (gx > 0, gx < sx - 1)
    has_y = (gy > 0, gy < sy - 1)
    to_x = ((gx - 1, gy), (gx + 1, gy))
    to_y = ((gx, gy - 1), (gx, gy + 1))
    barrier = pltpu.get_barrier_semaphore()
    for has, to in zip(has_x + has_y, to_x + to_y):
        @pl.when(has)
        def _():
            pl.semaphore_signal(barrier, inc=1, device_id=to, device_id_type=MESH)

    edges = pairs_of(ny)
    order = [y for pair in edges for y in pair]
    slot = {y: at + 1 for at, y in enumerate(order)} | {-1: 0, ny: ny + 1}
    wide = len(edges[0])

    cut = (len(edges) + 1) // 2
    halves = [edges[:cut], edges[cut:]] if edges[cut:] else [edges]
    columns = [[y for pair in half for y in pair] for half in halves]
    pieces = [pl.ds(slot[half[0]], len(half)) for half in columns]
    sides = sorted({0, nx - 1})
    middle = list(range(1, nx - 1))
    free = [(x, y) for y in order[wide:] for x in middle]
    rim = [(x, y) for y in order[:wide] for x in middle]
    face = [(x, y) for y in order for x in sides]
    corner = wide * len(sides)
    groups = [([(x, y) for y in order], (pl.ds(x + 1, 1), pl.ds(1, ny))) for x in sides]
    groups += [(rim, (pl.ds(2, nx - 2), pl.ds(1, wide))), (free, (pl.ds(2, nx - 2), pl.ds(1 + wide, ny - wide)))]
    groups = [group for group in groups if group[0]]
    kind = {cell: i for i, (cells, _) in enumerate(groups) for cell in cells}
    for x, y in face[:corner] + rim + face[corner:] + free:
        pltpu.make_async_copy(
            species_hbm.at[:, x, y], ext.at[x + 1, slot[y], real], load_sem.at[kind[x, y]]).start()

    def loaded(i):
        box = groups[i][1]
        pltpu.make_async_copy(
            ext2.at[box[0], box[1], real], ext.at[box[0], box[1], real], load_sem.at[i]).wait()

    small = [
        pltpu.make_async_copy(src, dst, small_sem.at[i]) for i, (src, dst) in enumerate((
            (mixing_hbm, mix), (inverses_hbm, inv), (diffusion_hbm, row),
            (rate_hbm, rates), (counts_hbm, counts), (class_hbm, classes)))]
    for copy in small:
        copy.start()

    tail = jnp.zeros((pad - spec, nz), F32)
    for x in range(nx + 2):
        for y in range(ny + 2):
            halo = x in (0, nx + 1) or y in (0, ny + 1)
            if x in (0, nx + 1) and y in (0, ny + 1):
                continue
            ext[x, y, pl.ds(spec, pad - spec)] = tail
            if halo:
                ext2[x, y, pl.ds(spec, pad - spec)] = tail
    blank = jnp.zeros((spec, nz), F32)
    for side in (0, 1):
        @pl.when(jnp.logical_not(has_x[side]))
        def _():
            for buf in (ext, ext2):
                for y in range(ny):
                    buf[side * (nx + 1), slot[y], real] = blank
        @pl.when(jnp.logical_not(has_y[side]))
        def _():
            for buf in (ext, ext2):
                for x in range(nx):
                    buf[x + 1, side * (ny + 1), real] = blank

    def x_copy(stage, side, c):
        buf = (ext, ext2)[stage]
        src_row, dst_row = (1, nx + 1) if side == 0 else (nx, 0)
        return pltpu.make_async_remote_copy(
            src_ref=buf.at[src_row, pieces[c], real],
            dst_ref=buf.at[dst_row, pieces[c], real],
            send_sem=xs_send.at[stage, side], recv_sem=xs_recv.at[side, stage * len(halves) + c],
            device_id=to_x[side], device_id_type=MESH)

    def x_face(stage, side):
        buf = (ext, ext2)[stage]
        rows = buf.at[1 if side == 0 else nx, pl.ds(1, ny), real]
        return pltpu.make_async_remote_copy(
            src_ref=rows, dst_ref=rows, send_sem=xs_send.at[stage, side],
            recv_sem=xs_recv.at[side, 0], device_id=to_x[side], device_id_type=MESH)

    def y_copy(stage, side):
        buf = (ext, ext2)[stage]
        src_col, dst_col = (slot[0], ny + 1) if side == 0 else (slot[ny - 1], 0)
        return pltpu.make_async_remote_copy(
            src_ref=buf.at[pl.ds(1, nx), src_col, real],
            dst_ref=buf.at[pl.ds(1, nx), dst_col, real],
            send_sem=ys_send.at[stage, side], recv_sem=ys_recv.at[stage, side],
            device_id=to_y[side], device_id_type=MESH)

    even = gx % 2 == 0
    near = (jnp.logical_not(even), even)

    def facing(close):
        for side in (0, 1):
            mine = near[side] if close else jnp.logical_not(near[side])
            yield side, jnp.logical_and(has_x[side], mine)

    def x_start(stage, close, cs=None):
        for side, there in facing(close):
            @pl.when(there)
            def _():
                for c in range(len(pieces)) if cs is None else cs:
                    x_copy(stage, side, c).start()

    def x_arrive(stage, close, c):
        for side, there in facing(close):
            @pl.when(there)
            def _():
                x_copy(stage, 1 - side, c).wait_recv()

    def y_start(stage):
        for side in (0, 1):
            @pl.when(has_y[side])
            def _():
                y_copy(stage, side).start()

    def y_arrive(stage):
        for side in (0, 1):
            @pl.when(has_y[side])
            def _():
                y_copy(stage, 1 - side).wait_recv()

    neighbours = sum(has.astype(jnp.int32) for has in has_x + has_y)
    pl.semaphore_wait(barrier, neighbours)
    for i in range(len(groups) - bool(free)):
        loaded(i)
    x_start(0, True)
    y_start(0)

    for copy in small:
        copy.wait()
    stack[...] = jnp.zeros_like(stack)
    square[...] = jnp.zeros_like(square)
    square[0:1, 0:spec] = row[...]
    line = jnp.broadcast_to(square[0:1, :], square.shape)
    on = lax.broadcasted_iota(jnp.int32, square.shape, 0) == lax.broadcasted_iota(
        jnp.int32, square.shape, 1)
    column = jnp.sum(jnp.where(on, line, 0.0), axis=1, keepdims=True)
    coef[...] = jnp.broadcast_to(column[:pad], coef.shape)
    square[0:spec, 0:spec] = mix[...]
    for k in range(nclass):
        stack[k * pad:k * pad + spec, 0:spec] = inv[:, k, :]
    mixed = jnp.dot(
        stack[...], square[...], precision=lax.Precision.HIGHEST, preferred_element_type=F32)
    spread = lax.broadcasted_iota(jnp.int32, (pad, 128), 1)
    highs, lows = [], []
    for k in range(nclass):
        rate = rates[k]
        own = stack[k * pad:(k + 1) * pad, :] * -(1.0 + rate)
        other = mixed[k * pad:(k + 1) * pad, :] * (rate * (1.0 + rate))
        both = own + pltpu.roll(other, pad, 1)
        high = both.astype(BF16).astype(F32)
        for part, into in ((high, highs), (both - high, lows)):
            turned = pltpu.roll(part, 2 * pad, 1)
            into.append(jnp.concatenate(
                [jnp.where(spread < 2 * pad, part, turned), turned], axis=1))
    for parts, ref in ((highs, w_high), (lows, w_low)):
        ref[...] = jnp.concatenate(
            [parts[k][t * 8:(t + 1) * 8] for t in range(pad // 8) for k in range(nclass)],
            axis=0)[:, :4 * pad].astype(BF16)

    lane = lax.broadcasted_iota(jnp.int32, (pad, nz), 1)

    def laplace(buf, x, y):
        at = slot[y]
        v = buf[x + 1, at]
        total = buf[x + 2, at] + buf[x, at] + buf[x + 1, slot[y + 1]] + buf[x + 1, slot[y - 1]]
        total = total + jnp.where(lane == nz - 1, 0.0, pltpu.roll(v, nz - 1, 1))
        total = total + jnp.where(lane == 0, 0.0, pltpu.roll(v, 1, 1))
        return v, total - 6.0 * v

    def solve(groups, hook):
        states, shrinks, whiches, limits = [], [], [], []
        for g, cells in enumerate(groups):
            parts = []
            for x, y in cells:
                v, lap = laplace(ext, x, y)
                force = coef[...] * lap
                out[x, y] = force
                parts.append(v + force)
            target = jnp.concatenate(parts, axis=1)
            which = jnp.concatenate([classes[pl.ds(x * ny + y, 1), :] for x, y in cells], axis=1)
            cell_rate = jnp.zeros(which.shape, F32)
            cell_count = jnp.zeros(which.shape, jnp.int32)
            for k in range(nclass):
                cell_rate = jnp.where(which == k, rates[k], cell_rate)
                cell_count = jnp.where(which == k, counts[k], cell_count)
            shrink = 1.0 / (1.0 + cell_rate)
            scaled[g, :, :target.shape[1]] = target * shrink
            states.append(target * cell_rate)
            shrinks.append(shrink)
            whiches.append(which)
            limits.append(cell_count)

        def value(g, state):
            return state * shrinks[g] + scaled[g, :, :state.shape[1]]

        def step(k, states):
            result = []
            for g, state in enumerate(states):
                z = jnp.concatenate([state, jnp.tanh(value(g, state))], axis=0)
                high = z.astype(BF16)
                low = (z - high.astype(F32)).astype(BF16)
                z = jnp.concatenate([high, low], axis=0)
                fixes = jnp.dot(w_high[...], z, preferred_element_type=F32)
                fixes = fixes + jnp.dot(w_low[...], z, preferred_element_type=F32)
                active = jnp.where(k < limits[g], whiches[g], nclass)
                picks = [active == n for n in range(nclass)]
                tiles = []
                for t in range(pad // 8):
                    fix = jnp.zeros((8, state.shape[1]), F32)
                    for n in range(nclass):
                        at = (t * nclass + n) * 8
                        fix = jnp.where(picks[n], fixes[at:at + 8], fix)
                    tiles.append(fix)
                result.append(state + jnp.concatenate(tiles, axis=0))
            return tuple(result)

        part = NMAX if hook is None else NMAX - 1
        states = lax.fori_loop(0, part, step, tuple(states), unroll=part)
        if hook is not None:
            hook()
            states = step(part, states)
        for g, (cells, state) in enumerate(zip(groups, states)):
            end = value(g, state)
            for i, (x, y) in enumerate(cells):
                ext2[x + 1, slot[y]] = end[:, i * nz:(i + 1) * nz]

    def pack(cells):
        return [cells[i:i + 2] for i in range(0, len(cells), 2)]

    def solve_all(cells, hook=None):
        groups = pack(cells)
        for i in range(0, len(groups), SPAN):
            solve(groups[i:i + SPAN], hook)
        if hook is not None and not groups:
            hook()

    if free:
        loaded(len(groups) - 1)
    near_x = (1 - gx % 2) * (nx - 1)
    far_x = nx - 1 - near_x
    first = 2 * (2 * len(free) // 6)
    solve_all(free[:first])
    solve_all(free[first:], lambda: x_start(0, False, [0]))
    y_arrive(0)
    for h in range(len(halves)):
        x_arrive(0, True, h)
    x_start(0, False, range(1, len(halves)))
    solve_all([(near_x, y) for y in order])
    x_start(1, True)
    for h, half in enumerate(columns):
        x_arrive(0, False, h)
        last = h == len(halves) - 1
        solve_all([(far_x, y) for y in half] + (rim if last else []))
        x_start(1, False, [h])
    y_start(1)

    def finish(x, y):
        v, lap = laplace(ext2, x, y)
        out[x, y] = v + 0.5 * (coef[...] * lap - out[x, y])

    def inside(x, y):
        at = slot[y]
        v = ext2[x + 1, at]
        total = ext2[jnp.where(x == 0, 2, nx - 1), at]
        total = total + ext2[x + 1, slot[y + 1]] + ext2[x + 1, slot[y - 1]]
        total = total + jnp.where(lane == nz - 1, 0.0, pltpu.roll(v, nz - 1, 1))
        total = total + jnp.where(lane == 0, 0.0, pltpu.roll(v, 1, 1))
        out[x, y] = v + 0.5 * (coef[...] * (total - 6.0 * v) - out[x, y])

    def across(x, y):
        out[x, y] = out[x, y] + 0.5 * coef[...] * ext2[jnp.where(x == 0, 0, nx + 1), slot[y]]

    for x, y in free:
        finish(x, y)
    for y in order[wide:]:
        for x in (near_x, far_x):
            inside(x, y)
    y_arrive(1)
    for x, y in rim:
        finish(x, y)
    for y in order[:wide]:
        for x in (near_x, far_x):
            inside(x, y)
    for close, x in ((False, far_x), (True, near_x)):
        for h, half in enumerate(columns):
            x_arrive(1, close, h)
            for y in half:
                across(x, y)

    for stage in (0, 1):
        for close in (True, False):
            for side, there in facing(close):
                @pl.when(there)
                def _():
                    x_face(stage, side).wait_send()
        for side in (0, 1):
            @pl.when(has_y[side])
            def _():
                y_copy(stage, side).wait_send()


def deliver(held, out_hbm, sem):
    spec, nx, ny, _ = out_hbm.shape
    copies = [
        pltpu.make_async_copy(held.at[x, y, pl.ds(0, spec)], out_hbm.at[:, x, y], sem)
        for x in range(nx) for y in range(ny)]
    for copy in copies:
        copy.start()
    every = held.at[:, :, pl.ds(0, spec)]
    pltpu.make_async_copy(every, every, sem).wait()


def local(species, diffusion, class_rate, mixing, inverses, newton_counts, cell_class):
    spec, nx, ny, nz = species.shape
    nclass = inverses.shape[0]
    pad = -(-spec // 8) * 8
    anywhere = pl.BlockSpec(memory_space=pl.ANY)
    vmem = pl.BlockSpec(memory_space=pltpu.VMEM)
    held = pl.pallas_call(
        functools.partial(kernel, (spec, nx, ny, nz, nclass)),
        out_shape=pltpu.VMEM((nx, ny, pad, nz), F32),
        in_specs=[anywhere] * 7,
        out_specs=vmem,
        scratch_shapes=[
            pltpu.VMEM((nx + 2, ny + 2, pad, nz), F32),
            pltpu.VMEM((nx + 2, ny + 2, pad, nz), F32),
            pltpu.VMEM((SPAN, pad, 2 * nz), F32),
            pltpu.VMEM((pad, nz), F32),
            pltpu.VMEM((1, spec), F32),
            pltpu.VMEM((spec, spec), F32),
            pltpu.VMEM((spec, nclass, spec), F32),
            pltpu.VMEM((nclass * pad, 128), F32),
            pltpu.VMEM((128, 128), F32),
            pltpu.VMEM((nclass * pad, 4 * pad), BF16),
            pltpu.VMEM((nclass * pad, 4 * pad), BF16),
            pltpu.VMEM((nx * ny, nz), jnp.int32),
            pltpu.SMEM((nclass,), F32),
            pltpu.SMEM((nclass,), jnp.int32),
            pltpu.SemaphoreType.DMA((4,)),
            pltpu.SemaphoreType.DMA((6,)),
            pltpu.SemaphoreType.DMA((2, 2)),
            pltpu.SemaphoreType.DMA((2, 4)),
            pltpu.SemaphoreType.DMA((2, 2)),
            pltpu.SemaphoreType.DMA((2, 2)),
        ],
        compiler_params=pltpu.CompilerParams(
            collective_id=0, has_side_effects=True, vmem_limit_bytes=60 * 1024 * 1024),
    )(
        species, diffusion.reshape(1, spec), class_rate,
        mixing, inverses.transpose(1, 0, 2), newton_counts, cell_class.reshape(nx * ny, nz),
    )
    return pl.pallas_call(
        deliver,
        out_shape=jax.ShapeDtypeStruct(species.shape, F32),
        in_specs=[vmem],
        out_specs=anywhere,
        scratch_shapes=[pltpu.SemaphoreType.DMA(())],
    )(pltpu.with_memory_space_constraint(held, pltpu.VMEM))


def solution(mesh):
    in_specs = (P(None, "gx", "gy", None), P(), P(), P(), P(), P(), P("gx", "gy", None))
    out_specs = P(None, "gx", "gy", None)
    return jax.shard_map(local, mesh=mesh, in_specs=in_specs, out_specs=out_specs, check_vma=False)
```

```python
import functools

import jax
import jax.numpy as jnp
from jax import lax
from jax.experimental import pallas as pl
from jax.experimental.pallas import tpu as pltpu
from jax.sharding import PartitionSpec as P

NMAX = 8
SPAN = 4
MESH = pl.DeviceIdType.MESH
F32 = jnp.float32
BF16 = jnp.bfloat16


def pairs_of(n):
    return [tuple(sorted({c, n - 1 - c})) for c in range((n + 1) // 2)]


def kernel(
    dims,
    species_hbm, diffusion_hbm, rate_hbm, mixing_hbm, inverses_hbm, counts_hbm, class_hbm,
    out,
    ext, ext2, scaled, coef, row, mix, inv, stack, square, w_high, w_low, classes, rates, counts,
    load_sem, small_sem, xs_send, xs_recv, ys_send, ys_recv,
):
    spec, nx, ny, nz, nclass = dims
    pad = ext.shape[2]
    real = pl.ds(0, spec)
    gx, gy = lax.axis_index("gx"), lax.axis_index("gy")
    sx, sy = lax.axis_size("gx"), lax.axis_size("gy")
    has_x = (gx > 0, gx < sx - 1)
    has_y = (gy > 0, gy < sy - 1)
    to_x = ((gx - 1, gy), (gx + 1, gy))
    to_y = ((gx, gy - 1), (gx, gy + 1))
    barrier = pltpu.get_barrier_semaphore()
    for has, to in zip(has_x + has_y, to_x + to_y):
        @pl.when(has)
        def _():
            pl.semaphore_signal(barrier, inc=1, device_id=to, device_id_type=MESH)

    edges = pairs_of(ny)
    order = [y for pair in edges for y in pair]
    slot = {y: at + 1 for at, y in enumerate(order)} | {-1: 0, ny: ny + 1}
    wide = len(edges[0])

    cut = (len(edges) + 1) // 2
    halves = [edges[:cut], edges[cut:]] if edges[cut:] else [edges]
    columns = [[y for pair in half for y in pair] for half in halves]
    pieces = [pl.ds(slot[half[0]], len(half)) for half in columns]
    sides = sorted({0, nx - 1})
    middle = list(range(1, nx - 1))
    free = [(x, y) for y in order[wide:] for x in middle]
    rim = [(x, y) for y in order[:wide] for x in middle]
    face = [(x, y) for y in order for x in sides]
    corner = wide * len(sides)
    groups = [([(x, y) for y in order], (pl.ds(x + 1, 1), pl.ds(1, ny))) for x in sides]
    groups += [(rim, (pl.ds(2, nx - 2), pl.ds(1, wide))), (free, (pl.ds(2, nx - 2), pl.ds(1 + wide, ny - wide)))]
    groups = [group for group in groups if group[0]]
    kind = {cell: i for i, (cells, _) in enumerate(groups) for cell in cells}
    for x, y in face[:corner] + rim + face[corner:] + free:
        pltpu.make_async_copy(
            species_hbm.at[:, x, y], ext.at[x + 1, slot[y], real], load_sem.at[kind[x, y]]).start()

    def loaded(i):
        box = groups[i][1]
        pltpu.make_async_copy(
            ext2.at[box[0], box[1], real], ext.at[box[0], box[1], real], load_sem.at[i]).wait()

    small = [
        pltpu.make_async_copy(src, dst, small_sem.at[i]) for i, (src, dst) in enumerate((
            (mixing_hbm, mix), (inverses_hbm, inv), (diffusion_hbm, row),
            (rate_hbm, rates), (counts_hbm, counts), (class_hbm, classes)))]
    for copy in small:
        copy.start()

    tail = jnp.zeros((pad - spec, nz), F32)
    for x in range(nx + 2):
        for y in range(ny + 2):
            halo = x in (0, nx + 1) or y in (0, ny + 1)
            if x in (0, nx + 1) and y in (0, ny + 1):
                continue
            ext[x, y, pl.ds(spec, pad - spec)] = tail
            if halo:
                ext2[x, y, pl.ds(spec, pad - spec)] = tail
    blank = jnp.zeros((spec, nz), F32)
    for side in (0, 1):
        @pl.when(jnp.logical_not(has_x[side]))
        def _():
            for buf in (ext, ext2):
                for y in range(ny):
                    buf[side * (nx + 1), slot[y], real] = blank
        @pl.when(jnp.logical_not(has_y[side]))
        def _():
            for buf in (ext, ext2):
                for x in range(nx):
                    buf[x + 1, side * (ny + 1), real] = blank

    def x_copy(stage, side, c):
        buf = (ext, ext2)[stage]
        src_row, dst_row = (1, nx + 1) if side == 0 else (nx, 0)
        return pltpu.make_async_remote_copy(
            src_ref=buf.at[src_row, pieces[c], real],
            dst_ref=buf.at[dst_row, pieces[c], real],
            send_sem=xs_send.at[side], recv_sem=xs_recv.at[side, stage * len(halves) + c],
            device_id=to_x[side], device_id_type=MESH)

    def x_face(stage, side):
        buf = (ext, ext2)[stage]
        rows = buf.at[1 if side == 0 else nx, pl.ds(1, ny), real]
        return pltpu.make_async_remote_copy(
            src_ref=rows, dst_ref=rows, send_sem=xs_send.at[side],
            recv_sem=xs_recv.at[side, 0], device_id=to_x[side], device_id_type=MESH)

    def y_copy(stage, side):
        buf = (ext, ext2)[stage]
        src_col, dst_col = (slot[0], ny + 1) if side == 0 else (slot[ny - 1], 0)
        return pltpu.make_async_remote_copy(
            src_ref=buf.at[pl.ds(1, nx), src_col, real],
            dst_ref=buf.at[pl.ds(1, nx), dst_col, real],
            send_sem=ys_send.at[side], recv_sem=ys_recv.at[stage, side],
            device_id=to_y[side], device_id_type=MESH)

    even = gx % 2 == 0
    near = (jnp.logical_not(even), even)

    def facing(close):
        for side in (0, 1):
            mine = near[side] if close else jnp.logical_not(near[side])
            yield side, jnp.logical_and(has_x[side], mine)

    def x_start(stage, close, cs=None):
        for side, there in facing(close):
            @pl.when(there)
            def _():
                for c in range(len(pieces)) if cs is None else cs:
                    x_copy(stage, side, c).start()

    def x_arrive(stage, close, c):
        for side, there in facing(close):
            @pl.when(there)
            def _():
                x_copy(stage, 1 - side, c).wait_recv()

    def x_sent(stage, close):
        for side, there in facing(close):
            @pl.when(there)
            def _():
                x_face(stage, side).wait_send()

    def y_sent(stage):
        for side in (0, 1):
            @pl.when(has_y[side])
            def _():
                y_copy(stage, side).wait_send()

    def y_start(stage):
        for side in (0, 1):
            @pl.when(has_y[side])
            def _():
                y_copy(stage, side).start()

    def y_arrive(stage):
        for side in (0, 1):
            @pl.when(has_y[side])
            def _():
                y_copy(stage, 1 - side).wait_recv()

    neighbours = sum(has.astype(jnp.int32) for has in has_x + has_y)
    pl.semaphore_wait(barrier, neighbours)
    for i in range(len(groups) - bool(free)):
        loaded(i)
    x_start(0, True)
    y_start(0)

    for copy in small:
        copy.wait()
    stack[...] = jnp.zeros_like(stack)
    square[...] = jnp.zeros_like(square)
    square[0:1, 0:spec] = row[...]
    line = jnp.broadcast_to(square[0:1, :], square.shape)
    on = lax.broadcasted_iota(jnp.int32, square.shape, 0) == lax.broadcasted_iota(
        jnp.int32, square.shape, 1)
    column = jnp.sum(jnp.where(on, line, 0.0), axis=1, keepdims=True)
    coef[...] = jnp.broadcast_to(column[:pad], coef.shape)
    square[0:spec, 0:spec] = mix[...]
    for k in range(nclass):
        stack[k * pad:k * pad + spec, 0:spec] = inv[:, k, :]
    mixed = jnp.dot(
        stack[...], square[...], precision=lax.Precision.HIGHEST, preferred_element_type=F32)
    spread = lax.broadcasted_iota(jnp.int32, (pad, 128), 1)
    highs, lows = [], []
    for k in range(nclass):
        rate = rates[k]
        own = stack[k * pad:(k + 1) * pad, :] * -(1.0 + rate)
        other = mixed[k * pad:(k + 1) * pad, :] * (rate * (1.0 + rate))
        both = own + pltpu.roll(other, pad, 1)
        high = both.astype(BF16).astype(F32)
        for part, into in ((high, highs), (both - high, lows)):
            turned = pltpu.roll(part, 2 * pad, 1)
            into.append(jnp.concatenate(
                [jnp.where(spread < 2 * pad, part, turned), turned], axis=1))
    for parts, ref in ((highs, w_high), (lows, w_low)):
        ref[...] = jnp.concatenate(
            [parts[k][t * 8:(t + 1) * 8] for t in range(pad // 8) for k in range(nclass)],
            axis=0)[:, :4 * pad].astype(BF16)

    lane = lax.broadcasted_iota(jnp.int32, (pad, nz), 1)

    def laplace(buf, x, y):
        at = slot[y]
        v = buf[x + 1, at]
        total = buf[x + 2, at] + buf[x, at] + buf[x + 1, slot[y + 1]] + buf[x + 1, slot[y - 1]]
        total = total + jnp.where(lane == nz - 1, 0.0, pltpu.roll(v, nz - 1, 1))
        total = total + jnp.where(lane == 0, 0.0, pltpu.roll(v, 1, 1))
        return v, total - 6.0 * v

    def solve(groups, hook):
        states, shrinks, whiches, limits = [], [], [], []
        for g, cells in enumerate(groups):
            parts = []
            for x, y in cells:
                v, lap = laplace(ext, x, y)
                force = coef[...] * lap
                out[x, y] = force
                parts.append(v + force)
            target = jnp.concatenate(parts, axis=1)
            which = jnp.concatenate([classes[pl.ds(x * ny + y, 1), :] for x, y in cells], axis=1)
            cell_rate = jnp.zeros(which.shape, F32)
            cell_count = jnp.zeros(which.shape, jnp.int32)
            for k in range(nclass):
                cell_rate = jnp.where(which == k, rates[k], cell_rate)
                cell_count = jnp.where(which == k, counts[k], cell_count)
            shrink = 1.0 / (1.0 + cell_rate)
            scaled[g, :, :target.shape[1]] = target * shrink
            states.append(target * cell_rate)
            shrinks.append(shrink)
            whiches.append(which)
            limits.append(cell_count)

        def value(g, state):
            return state * shrinks[g] + scaled[g, :, :state.shape[1]]

        def step(k, states):
            result = []
            for g, state in enumerate(states):
                z = jnp.concatenate([state, jnp.tanh(value(g, state))], axis=0)
                high = z.astype(BF16)
                low = (z - high.astype(F32)).astype(BF16)
                z = jnp.concatenate([high, low], axis=0)
                fixes = jnp.dot(w_high[...], z, preferred_element_type=F32)
                fixes = fixes + jnp.dot(w_low[...], z, preferred_element_type=F32)
                active = jnp.where(k < limits[g], whiches[g], nclass)
                picks = [active == n for n in range(nclass)]
                tiles = []
                for t in range(pad // 8):
                    fix = jnp.zeros((8, state.shape[1]), F32)
                    for n in range(nclass):
                        at = (t * nclass + n) * 8
                        fix = jnp.where(picks[n], fixes[at:at + 8], fix)
                    tiles.append(fix)
                result.append(state + jnp.concatenate(tiles, axis=0))
            return tuple(result)

        part = NMAX if hook is None else NMAX - 1
        states = lax.fori_loop(0, part, step, tuple(states), unroll=part)
        if hook is not None:
            hook()
            states = step(part, states)
        for g, (cells, state) in enumerate(zip(groups, states)):
            end = value(g, state)
            for i, (x, y) in enumerate(cells):
                ext2[x + 1, slot[y]] = end[:, i * nz:(i + 1) * nz]

    def pack(cells):
        return [cells[i:i + 2] for i in range(0, len(cells), 2)]

    def solve_all(cells, hook=None):
        groups = pack(cells)
        for i in range(0, len(groups), SPAN):
            solve(groups[i:i + SPAN], hook)
        if hook is not None and not groups:
            hook()

    if free:
        loaded(len(groups) - 1)
    near_x = (1 - gx % 2) * (nx - 1)
    far_x = nx - 1 - near_x
    first = 2 * (2 * len(free) // 6)
    solve_all(free[:first])
    solve_all(free[first:], lambda: x_start(0, False, [0]))
    y_arrive(0)
    for h in range(len(halves)):
        x_arrive(0, True, h)
    x_start(0, False, range(1, len(halves)))
    solve_all([(near_x, y) for y in order])
    x_sent(0, True)
    x_start(1, True)
    for h, half in enumerate(columns):
        x_arrive(0, False, h)
        last = h == len(halves) - 1
        solve_all([(far_x, y) for y in half] + (rim if last else []))
        if h == 0:
            x_sent(0, False)
        x_start(1, False, [h])
    y_sent(0)
    y_start(1)

    def finish(x, y):
        v, lap = laplace(ext2, x, y)
        out[x, y] = v + 0.5 * (coef[...] * lap - out[x, y])

    def inside(x, y):
        at = slot[y]
        v = ext2[x + 1, at]
        total = ext2[jnp.where(x == 0, 2, nx - 1), at]
        total = total + ext2[x + 1, slot[y + 1]] + ext2[x + 1, slot[y - 1]]
        total = total + jnp.where(lane == nz - 1, 0.0, pltpu.roll(v, nz - 1, 1))
        total = total + jnp.where(lane == 0, 0.0, pltpu.roll(v, 1, 1))
        out[x, y] = v + 0.5 * (coef[...] * (total - 6.0 * v) - out[x, y])

    def across(x, y):
        out[x, y] = out[x, y] + 0.5 * coef[...] * ext2[jnp.where(x == 0, 0, nx + 1), slot[y]]

    for x, y in free:
        finish(x, y)
    for y in order[wide:]:
        for x in (near_x, far_x):
            inside(x, y)
    y_arrive(1)
    for x, y in rim:
        finish(x, y)
    for y in order[:wide]:
        for x in (near_x, far_x):
            inside(x, y)
    for close, x in ((False, far_x), (True, near_x)):
        for h, half in enumerate(columns):
            x_arrive(1, close, h)
            for y in half:
                across(x, y)

    x_sent(1, True)
    x_sent(1, False)
    y_sent(1)


def deliver(held, out_hbm, sem):
    spec, nx, ny, _ = out_hbm.shape
    copies = [
        pltpu.make_async_copy(held.at[x, y, pl.ds(0, spec)], out_hbm.at[:, x, y], sem)
        for x in range(nx) for y in range(ny)]
    for copy in copies:
        copy.start()
    every = held.at[:, :, pl.ds(0, spec)]
    pltpu.make_async_copy(every, every, sem).wait()


def local(species, diffusion, class_rate, mixing, inverses, newton_counts, cell_class):
    spec, nx, ny, nz = species.shape
    nclass = inverses.shape[0]
    pad = -(-spec // 8) * 8
    anywhere = pl.BlockSpec(memory_space=pl.ANY)
    vmem = pl.BlockSpec(memory_space=pltpu.VMEM)
    held = pl.pallas_call(
        functools.partial(kernel, (spec, nx, ny, nz, nclass)),
        out_shape=pltpu.VMEM((nx, ny, pad, nz), F32),
        in_specs=[anywhere] * 7,
        out_specs=vmem,
        scratch_shapes=[
            pltpu.VMEM((nx + 2, ny + 2, pad, nz), F32),
            pltpu.VMEM((nx + 2, ny + 2, pad, nz), F32),
            pltpu.VMEM((SPAN, pad, 2 * nz), F32),
            pltpu.VMEM((pad, nz), F32),
            pltpu.VMEM((1, spec), F32),
            pltpu.VMEM((spec, spec), F32),
            pltpu.VMEM((spec, nclass, spec), F32),
            pltpu.VMEM((nclass * pad, 128), F32),
            pltpu.VMEM((128, 128), F32),
            pltpu.VMEM((nclass * pad, 4 * pad), BF16),
            pltpu.VMEM((nclass * pad, 4 * pad), BF16),
            pltpu.VMEM((nx * ny, nz), jnp.int32),
            pltpu.SMEM((nclass,), F32),
            pltpu.SMEM((nclass,), jnp.int32),
            pltpu.SemaphoreType.DMA((4,)),
            pltpu.SemaphoreType.DMA((6,)),
            pltpu.SemaphoreType.DMA((2,)),
            pltpu.SemaphoreType.DMA((2, 4)),
            pltpu.SemaphoreType.DMA((2,)),
            pltpu.SemaphoreType.DMA((2, 2)),
        ],
        compiler_params=pltpu.CompilerParams(
            collective_id=0, has_side_effects=True, vmem_limit_bytes=60 * 1024 * 1024),
    )(
        species, diffusion.reshape(1, spec), class_rate,
        mixing, inverses.transpose(1, 0, 2), newton_counts, cell_class.reshape(nx * ny, nz),
    )
    return pl.pallas_call(
        deliver,
        out_shape=jax.ShapeDtypeStruct(species.shape, F32),
        in_specs=[vmem],
        out_specs=anywhere,
        scratch_shapes=[pltpu.SemaphoreType.DMA(())],
    )(pltpu.with_memory_space_constraint(held, pltpu.VMEM))


def solution(mesh):
    in_specs = (P(None, "gx", "gy", None), P(), P(), P(), P(), P(), P("gx", "gy", None))
    out_specs = P(None, "gx", "gy", None)
    return jax.shard_map(local, mesh=mesh, in_specs=in_specs, out_specs=out_specs, check_vma=False)
```
